32 devices in a mesh: rows: 8 (over y, x, core), planes: 4 (over z).
Axes of the slice: x: 2, y: 2, z: 4, core: 2. Of those that a mesh axis runs over, the one named last changes fastest.
Arguments:
- density: float32 [4, 4096, 4096], P('planes', 'rows'), may hold values from -6 to 6
- lens_weight: float32 [4], P('planes'), may hold values from 0.05 to 0.5
- spectrum_bin: int32 [4096, 4096], P(None, ('rows', 'planes')), may hold values from 0 to 63, as said below
Outputs:
- shear_real: float32 [4096, 4096], P(('rows', 'planes'))
- shear_imag: float32 [4096, 4096], P(('rows', 'planes'))
- spectrum: float32 [64], replicated
The draws below stay inside these ranges and needn't reach their ends.
Inputs may be any that keep to these rules, and one draw needn't show every extreme that they name: `spectrum_bin`: each Fourier pixel's band.
All inputs are finite; a program needn't handle non-finite values.
Results may differ from the reference program's by a relative error of at most 0.0003.
Values sent between devices are 32-bit elements; how exact they have to be, the bound alone decides.
A program may use at most 64 MiB of HBM per device.

```python
import math
import jax
import jax.numpy as jnp
from jax import lax

N = 4096
NBINS = 64
PLANES = 4


def draw_spectrum_bin(key, part):
    frequency = (jnp.arange(N, dtype=jnp.int32) + N // 2) % N - N // 2
    square_norm = frequency[:, None] ** 2 + frequency[None, :] ** 2
    radial = jnp.minimum(square_norm * NBINS // (N * N // 2), NBINS - 1)
    jitter = jax.random.randint(key, (N, N), -1, 2, dtype=jnp.int32)
    return jnp.clip(radial + jitter, 0, NBINS - 1).astype(jnp.int32)


def level_of(rng, shape, cuts, least, high):
    level = 1.0
    for axis_at, parts in cuts:
        draws = jax.random.uniform(jax.random.fold_in(jax.random.fold_in(rng, 6), axis_at), (parts,), jnp.float32, least / len(cuts), high / len(cuts))
        level = level * jnp.repeat(jnp.exp(draws), shape[axis_at] // parts).reshape((-1,) + (1,) * (len(shape) - 1 - axis_at))
    return level


def bell_draw(rng, dims, spread, limit, cuts=(), held_as=jnp.bfloat16):
    entries = spread * jax.random.normal(rng, dims, jnp.float32)
    if cuts:
        entries = entries * level_of(rng, dims, cuts, -0.22, 0.18)
    return jnp.clip(entries, -limit, limit).astype(held_as)


def setup_inputs(seed: int = 0) -> dict:
    keys = jax.random.split(jax.random.key(seed), 4)
    return {
        "density": bell_draw(keys[0], (PLANES, N, N), 1.0, 6.0, ((0, 4), (1, 8)), jnp.float32),
        "lens_weight": jnp.clip(jnp.exp(math.log(0.5) - 2.3025851 * jax.random.uniform(keys[1], (PLANES,), jnp.float32) ** level_of(keys[1], (PLANES,), ((0, 4),), -0.2, 0.2)), 0.05, 0.5),
        "spectrum_bin": draw_spectrum_bin(jax.random.fold_in(keys[3], 71), 0),
    }


def reference(density, lens_weight, spectrum_bin):
    def accumulate(plane_index, running):
        total_real, total_imag = running
        weighted_plane = density[plane_index] * lens_weight[plane_index]
        plane_hat = jnp.fft.fft2(weighted_plane)
        return (total_real + jnp.real(plane_hat), total_imag + jnp.imag(plane_hat))

    empty_sum = jnp.zeros((N, N), jnp.float32)
    total_real, total_imag = lax.fori_loop(0, PLANES, accumulate, (empty_sum, empty_sum))
    frequency = ((jnp.arange(N, dtype=jnp.int32) + N // 2) % N - N // 2).astype(jnp.float32)
    height = frequency[:, None]
    across = frequency[None, :]
    square_norm = height ** 2 + across ** 2
    anchor = square_norm == 0
    safe_norm = jnp.where(anchor, 1.0, square_norm)
    total_real = jnp.where(anchor, 0.0, total_real)
    total_imag = jnp.where(anchor, 0.0, total_imag)
    pixel_power = (total_real ** 2 + total_imag ** 2) * (NBINS / float(N) ** 4)
    spectrum = jax.ops.segment_sum(pixel_power.reshape(-1), spectrum_bin.reshape(-1), num_segments=NBINS)
    kernel_real = (across ** 2 - height ** 2) / safe_norm
    kernel_imag = 2.0 * across * height / safe_norm
    hat_real = kernel_real * total_real - kernel_imag * total_imag
    hat_imag = kernel_real * total_imag + kernel_imag * total_real
    shear_field = jnp.fft.ifft2(hat_real + 1j * hat_imag)
    return jnp.real(shear_field).astype(jnp.float32), jnp.imag(shear_field).astype(jnp.float32), spectrum
```

```python
import functools
import math

import jax
import jax.numpy as jnp
import numpy as np
from jax import lax
from jax.experimental import pallas as pl
from jax.experimental.pallas import tpu as pltpu
from jax.sharding import PartitionSpec as P

NBINS = 64
AXES = ("rows", "planes")
LANES = 128
HALF = LANES // 2
TILE = 8
MESH = pl.DeviceIdType.MESH
F32 = jnp.float32
BF16 = jnp.bfloat16


def real_fft(xs):
    n = len(xs)
    if n == 2:
        return [(xs[0] + xs[1], None), (xs[0] - xs[1], None)]
    even, odd = real_fft(xs[0::2]), real_fft(xs[1::2])
    out = [None] * (n // 2 + 1)
    out[0] = (even[0][0] + odd[0][0], None)
    out[n // 2] = (even[0][0] - odd[0][0], None)
    out[n // 4] = (even[n // 4][0], -odd[n // 4][0])
    for k in range(1, n // 4):
        c, s = math.cos(2 * math.pi * k / n), math.sin(2 * math.pi * k / n)
        (er, ei), (odr, odi) = even[k], odd[k]
        tr, ti = c * odr + s * odi, c * odi - s * odr
        out[k] = (er + tr, ei + ti)
        out[n // 2 - k] = (er - tr, ti - ei)
    return out


def real_inverse(spec, n):
    if n == 2:
        return [spec[0][0] + spec[1][0], spec[0][0] - spec[1][0]]
    h, q = n // 2, n // 4
    even, odd = [None] * (q + 1), [None] * (q + 1)
    even[0] = (spec[0][0] + spec[h][0], None)
    odd[0] = (spec[0][0] - spec[h][0], None)
    even[q] = (2.0 * spec[q][0], None)
    odd[q] = (-2.0 * spec[q][1], None)
    for k in range(1, q):
        (ar, ai), (br, bi) = spec[k], spec[h - k]
        even[k] = (ar + br, ai - bi)
        ur, ui = ar - br, ai + bi
        c, s = math.cos(2 * math.pi * k / n), math.sin(2 * math.pi * k / n)
        odd[k] = (c * ur - s * ui, c * ui + s * ur)
    evens, odds = real_inverse(even, h), real_inverse(odd, h)
    out = [None] * n
    out[0::2], out[1::2] = evens, odds
    return out


def packed_fft(xs, orient, times_i):
    n = len(xs)
    if n == 1:
        return xs
    even = packed_fft(xs[0::2], orient, times_i)
    odd = packed_fft(xs[1::2], orient, times_i)
    out = [None] * n
    for k in range(n // 2):
        c, s = math.cos(2 * math.pi * k / n), orient * math.sin(2 * math.pi * k / n)
        if k == 0:
            t = odd[0]
        elif 4 * k == n:
            t = times_i(odd[k]) * float(orient)
        else:
            t = c * odd[k] + s * times_i(odd[k])
        out[k], out[k + n // 2] = even[k] + t, even[k] - t
    return out


def split(x):
    high = x.astype(BF16)
    return high, (x - high.astype(F32)).astype(BF16)


def dot3(left, right):
    lh, ll = split(left)
    rh, rl = split(right)
    return jnp.dot(
        jnp.concatenate([lh, lh, ll], 1),
        jnp.concatenate([rh, rl, rh], 0),
        preferred_element_type=F32,
    )


def row_tables(fold):
    length = fold * LANES
    a = np.arange(LANES)
    general = np.zeros((2, LANES, 2, 2, HALF))
    special = np.zeros((2, LANES, 2, 2, HALF))
    for h in range(2):
        m = h * HALF + np.arange(HALF)
        angle = 2 * np.pi * (a[:, None] * m[None, :] % LANES) / LANES
        general[0, :, h, 0], general[0, :, h, 1] = np.cos(angle), -np.sin(angle)
        general[1, :, h, 0], general[1, :, h, 1] = np.sin(angle), np.cos(angle)
        kx = fold * np.arange(HALF) + h * (fold // 2)
        angle = 2 * np.pi * (a[:, None] * kx[None, :] % length) / length
        special[h, :, h, 0], special[h, :, h, 1] = np.cos(angle), -np.sin(angle)
    special[0, :, 0, 1, 0] = 1 - 2 * (a % 2)
    shape = (2 * LANES, 2 * LANES)
    return general.reshape(shape).astype(np.float32), special.reshape(shape).astype(np.float32)


def back_tables(fold):
    length = fold * LANES
    a = np.arange(LANES)
    general = np.zeros((2, 2, HALF, 2, LANES))
    special = np.zeros((2, 2, HALF, 2, LANES))
    for h in range(2):
        m = h * HALF + np.arange(HALF)
        angle = 2 * np.pi * (m[:, None] * a[None, :] % LANES) / LANES
        general[h, 0, :, 0], general[h, 0, :, 1] = np.cos(angle), np.sin(angle)
        general[h, 1, :, 0], general[h, 1, :, 1] = -np.sin(angle), np.cos(angle)
        kx = fold * np.arange(HALF) + h * (fold // 2)
        angle = 2 * np.pi * (kx[:, None] * a[None, :] % length) / length
        special[h, 0, :, h], special[h, 1, :, h] = 2 * np.cos(angle), -2 * np.sin(angle)
    special[0, 0, 0, 0] = 1.0
    special[0, 1, 0, 0] = 1 - 2 * (a % 2)
    shape, scale = (2 * LANES, 2 * LANES), float(length) ** -2
    return (
        (general.reshape(shape) * scale).astype(np.float32),
        (special.reshape(shape) * scale).astype(np.float32),
    )


def column_table():
    a = np.arange(LANES)
    angle = 2 * np.pi * (a[:, None] * a[None, :] % LANES) / LANES
    return np.concatenate([np.cos(angle), np.sin(angle)], 1).astype(np.float32)


def turn_table(length):
    angle = 2 * np.pi * np.arange(LANES)[:, None] / length * np.ones((1, LANES))
    return np.stack([np.cos(angle), np.sin(angle)]).astype(np.float32)


def shear_kernel(
    rows, planes, slab,
    density, weight, bins, row_base, row_zero, back_base, back_zero, column, turns,
    out_real, out_imag, out_spectrum,
    staged, folded, parts, from_low, from_high, lines, hat, shear, power, arrived,
    bins_in, bands, sums, sums_out, sums_in, table,
    stage_sem, low_send, low_recv, high_send, high_recv, cross_send, cross_recv,
    bins_send, bins_recv, bins_own, turn_send, turn_recv, sum_send, sum_recv,
):
    devices = rows * planes
    fold = devices
    length = fold * LANES
    slots = fold // 2
    blocks = slab // LANES
    pairs = planes // 2
    angle_unit = 2 * math.pi / length
    r, p = lax.axis_index("rows"), lax.axis_index("planes")
    me = r * planes + p

    def place(device):
        return {"rows": device // planes, "planes": lax.rem(device, planes)}

    lane = lax.broadcasted_iota(jnp.int32, (1, LANES), 1)
    sign = jnp.where(lane < HALF, -1.0, 1.0)

    def times_i(x):
        return pltpu.roll(x, HALF, axis=1) * sign

    def minus_i(x):
        return pltpu.roll(x, HALF, axis=1) * (-sign)

    barrier = pltpu.get_barrier_semaphore()
    for step in range(1, devices):
        pl.semaphore_signal(
            barrier, inc=1, device_id=place(lax.rem(me + step, devices)), device_id_type=MESH
        )

    depth = staged.shape[1]
    chunks = slab // depth

    def stage(c):
        slot = lax.rem(c, 2)
        return pltpu.make_async_copy(
            density.at[pl.ds(c * depth, depth)], staged.at[slot], stage_sem.at[slot]
        )

    stage(0).start()
    scale = weight[0]

    def stage_step(c, carry):
        @pl.when(c + 1 < chunks)
        def _():
            stage(c + 1).start()

        stage(c).wait()
        slot = lax.rem(c, 2)

        def tile(i, carry):
            take = pl.ds(pl.multiple_of(i * TILE, TILE), TILE)
            xs = [staged[slot, take, b * LANES:(b + 1) * LANES] * scale for b in range(fold)]
            spec = real_fft(xs)
            put = pl.ds(pl.multiple_of(c * depth + i * TILE, TILE), TILE)
            folded[0, put, :LANES] = spec[0][0]
            folded[0, put, LANES:] = spec[slots][0]
            for k in range(1, slots):
                folded[k, put, :LANES] = spec[k][0]
                folded[k, put, LANES:] = spec[k][1]
            return carry

        return lax.fori_loop(0, depth // TILE, tile, carry)

    lax.fori_loop(0, chunks, stage_step, 0)
    pl.semaphore_wait(barrier, devices - 1)

    def up(dest, owner):
        return pltpu.make_async_remote_copy(
            parts.at[dest, owner], from_low.at[dest, owner - 1],
            low_send.at[dest, owner - 1], low_recv.at[dest, owner - 1],
            device_id={"rows": r, "planes": lax.rem(p + 1, planes)}, device_id_type=MESH,
        )

    def down(dest, owner):
        return pltpu.make_async_remote_copy(
            parts.at[dest, owner], from_high.at[dest, owner],
            high_send.at[dest, owner], high_recv.at[dest, owner],
            device_id={"rows": r, "planes": lax.rem(p + planes - 1, planes)},
            device_id_type=MESH,
        )

    def cross(dest):
        return pltpu.make_async_remote_copy(
            parts.at[dest, p], lines.at[pl.ds(r * blocks, blocks)],
            cross_send.at[dest], cross_recv.at[r],
            device_id={"rows": dest, "planes": p}, device_id_type=MESH,
        )

    def crossed(source):
        return pltpu.make_async_remote_copy(
            parts.at[source, p], lines.at[pl.ds(source * blocks, blocks)],
            cross_send.at[source], cross_recv.at[source],
            device_id={"rows": source, "planes": p}, device_id_type=MESH,
        )

    at_a = lax.broadcasted_iota(jnp.int32, (LANES, LANES), 0)

    def row_step(i, carry):
        dest = lax.rem(r + 1 + i, rows)
        for pair in range(pairs):
            k = dest * pairs + pair
            angle = (at_a * k).astype(F32) * angle_unit
            c, s = jnp.cos(angle), jnp.sin(angle)
            c, s = jnp.concatenate([c, c], 1), jnp.concatenate([s, s], 1)
            top, low = row_base[:LANES], row_base[LANES:]
            table[:LANES] = c * top - s * low
            table[LANES:] = c * low + s * top

            @pl.when(k == 0)
            def _():
                table[...] = row_zero[...]

            right = table[...]
            for q in range(blocks):
                done = dot3(folded[k, q * LANES:(q + 1) * LANES], right)
                parts[dest, 2 * pair, q] = done[:, :LANES]
                parts[dest, 2 * pair + 1, q] = done[:, LANES:]

        @pl.when(p == 0)
        def _():
            for owner in range(planes - 1, 0, -1):
                up(dest, owner).start()

        @pl.when(p == planes - 1)
        def _():
            for owner in range(planes - 1):
                down(dest, owner).start()

        return carry

    lax.fori_loop(0, rows, row_step, 0)

    side = me // slots

    def class_at(owner):
        k, h = owner // 2, lax.rem(owner, 2)
        other = k + lax.rem(h + side, 2) * (fold - 2 * k)
        return jnp.where(k == 0, h * slots, other)

    def send_bins(step):
        owner = lax.rem(me + step, devices)
        return pltpu.make_async_remote_copy(
            bins.at[class_at(owner)], bins_in.at[me],
            bins_send.at[step], bins_recv.at[step],
            device_id=place(owner), device_id_type=MESH,
        )

    def recv_bins(step):
        source = lax.rem(me + devices - step, devices)
        return pltpu.make_async_remote_copy(
            bins.at[0], bins_in.at[source],
            bins_send.at[step], bins_recv.at[step],
            device_id=place(source), device_id_type=MESH,
        )

    own_bins = pltpu.make_async_copy(bins.at[class_at(me)], bins_in.at[me], bins_own)
    own_bins.start()

    def bins_step(step, carry):
        send_bins(step).start()
        return carry

    lax.fori_loop(1, devices, bins_step, 0)

    def sum_step(i, carry):
        dest = lax.rem(r + 1 + i, rows)
        for back in range(planes - 1):
            owner = planes - 1 - back

            @pl.when((p >= 1) & (p <= owner))
            def _():
                up(dest, owner).wait_recv()
                parts[dest, owner] = parts[dest, owner] + from_low[dest, owner - 1]

            @pl.when((p >= 1) & (p < owner))
            def _():
                up(dest, owner).start()

            owner_down = back

            @pl.when((p <= planes - 2) & (p >= owner_down))
            def _():
                down(dest, owner_down).wait_recv()
                parts[dest, owner_down] = parts[dest, owner_down] + from_high[dest, owner_down]

            @pl.when((p <= planes - 2) & (p > owner_down))
            def _():
                down(dest, owner_down).start()

        @pl.when(dest != r)
        def _():
            cross(dest).start()

        return carry

    lax.fori_loop(0, rows, sum_step, 0)

    def own_step(q, carry):
        lines[r * blocks + q] = parts[r, p, q]
        return carry

    lax.fori_loop(0, blocks, own_step, 0)

    def crossed_step(i, carry):
        crossed(lax.rem(r + rows - 1 - i, rows)).wait_recv()
        return carry

    lax.fori_loop(0, rows - 1, crossed_step, 0)

    def column_tile(i, carry):
        take = pl.ds(pl.multiple_of(i * TILE, TILE), TILE)
        spec = packed_fft([lines[b, take] for b in range(fold)], -1, times_i)
        for k in range(fold):
            lines[k, take] = spec[k]
        return carry

    lax.fori_loop(0, LANES // TILE, column_tile, 0)

    k_me, h_me = me // 2, lax.rem(me, 2)
    index = lax.rem(lane, HALF)
    kx = jnp.where(
        k_me == 0, fold * index + h_me * slots, fold * (HALF * h_me + index) + k_me
    )
    across = jnp.where(kx >= length // 2, kx - length, kx).astype(F32)
    my = lax.broadcasted_iota(jnp.int32, (LANES, LANES), 0)
    at_lane = lax.broadcasted_iota(jnp.int32, (LANES, LANES), 1)
    pixel_scale = NBINS / float(length) ** 4

    def height_of(k):
        ky = k + fold * my
        return jnp.where(ky >= length // 2, ky - length, ky).astype(F32)

    def kernel_of(width, height):
        square_norm = height * height + width * width
        safe = jnp.where(square_norm == 0.0, 1.0, square_norm)
        inverse = 1.0 / safe
        return (width * width - height * height) * inverse, 2.0 * width * height * inverse

    def edge_of(k):
        return (my == HALF) & (k == 0)

    def column_step(k, carry):
        angle = (lane * k).astype(F32) * angle_unit
        c, s = jnp.cos(angle), jnp.sin(angle)
        cos, sin = column[:, :LANES], column[:, LANES:]
        left = jnp.concatenate([cos * c - sin * s, sin * c + cos * s], 1)
        z = lines[k]
        v = dot3(left, jnp.concatenate([z, minus_i(z)], 0))
        hat[k] = v
        square = v * v
        power[k] = (square + pltpu.roll(square, HALF, axis=1)) * pixel_scale
        kernel_real, kernel_imag = kernel_of(across, height_of(k))
        edge = edge_of(k)
        shear[k, :, :LANES] = kernel_real * v + jnp.where(edge, kernel_imag * times_i(v), 0.0)
        shear[k, :, LANES:] = jnp.where(edge, 0.0, kernel_imag * v)
        return carry

    lax.fori_loop(0, fold, column_step, 0)

    def reverse_of(k):
        wrapped = jnp.where(k == 0, LANES - my, LANES - 1 - my)
        return jnp.where(lax.rem(wrapped, LANES) == at_lane, 1.0, 0.0).astype(BF16)

    @pl.when(me == 0)
    def _():
        def repair(k, carry):
            v = hat[k]
            high, low = split(hat[lax.rem(fold - k, fold)])
            reverse = reverse_of(k)
            mirror = jnp.dot(reverse, high, preferred_element_type=F32) + jnp.dot(
                reverse, low, preferred_element_type=F32
            )
            mirror = mirror * (-sign)
            zero = (v + mirror) * 0.5
            zero = jnp.where((my == 0) & (k == 0), 0.0, zero)
            last = minus_i((v - mirror) * 0.5)
            zero_square, last_square = zero * zero, last * last
            zero_power = (zero_square + pltpu.roll(zero_square, HALF, axis=1)) * pixel_scale
            last_power = (last_square + pltpu.roll(last_square, HALF, axis=1)) * pixel_scale
            held = jnp.where(at_lane == HALF, last_power, power[k])
            power[k] = jnp.where(at_lane == 0, zero_power, held)
            height = height_of(k)
            kernel_real, kernel_imag = kernel_of(float(-(length // 2)), height)
            turned = times_i(kernel_real * last + kernel_imag * times_i(last))
            edge = edge_of(k)
            first = (at_lane == 0) | (at_lane == HALF)
            real = jnp.where(edge, 0.0, turned) - zero
            imag = jnp.where(edge, times_i(last), 0.0)
            shear[k, :, :LANES] = jnp.where(first, real, shear[k, :, :LANES])
            shear[k, :, LANES:] = jnp.where(first, imag, shear[k, :, LANES:])
            return carry

        lax.fori_loop(0, fold, repair, 0)

    table[:LANES] = column[...]

    def inverse_step(k, carry):
        real, imag = shear[k, :, :LANES], shear[k, :, LANES:]
        top = jnp.concatenate([real, imag], 1)
        low = jnp.concatenate([times_i(real), times_i(imag)], 1)
        shear[k] = dot3(table[:LANES], jnp.concatenate([top, low], 0))
        cos, sin = table[:LANES, :LANES], table[:LANES, LANES:]
        c, s = turns[0], turns[1]
        table[:LANES, :LANES] = cos * c - sin * s
        table[:LANES, LANES:] = sin * c + cos * s
        return carry

    lax.fori_loop(0, fold, inverse_step, 0)

    def inverse_tile(i, carry):
        take = pl.ds(pl.multiple_of(i * TILE, TILE), TILE)
        for part in range(2):
            span = slice(part * LANES, (part + 1) * LANES)
            lines_out = packed_fft([shear[k, take, span] for k in range(fold)], 1, times_i)
            for b in range(fold):
                shear[b, take, span] = lines_out[b]
        return carry

    lax.fori_loop(0, LANES // TILE, inverse_tile, 0)

    def give(step):
        dest = lax.rem(me + step, devices)
        return pltpu.make_async_remote_copy(
            shear.at[dest], arrived.at[me], turn_send.at[step], turn_recv.at[step],
            device_id=place(dest), device_id_type=MESH,
        )

    def got(step):
        source = lax.rem(me + devices - step, devices)
        return pltpu.make_async_remote_copy(
            shear.at[source], arrived.at[source], turn_send.at[step], turn_recv.at[step],
            device_id=place(source), device_id_type=MESH,
        )

    def give_step(step, carry):
        give(step).start()
        return carry

    lax.fori_loop(1, devices, give_step, 0)
    arrived[me] = shear[me]

    own_bins.wait()

    def bins_wait(step, carry):
        recv_bins(step).wait_recv()
        return carry

    lax.fori_loop(1, devices, bins_wait, 0)

    at_row = lax.broadcasted_iota(jnp.int32, (2 * LANES, 2 * LANES), 0)
    at_column = lax.broadcasted_iota(jnp.int32, (2 * LANES, 2 * LANES), 1)
    which = lax.rem(at_row // 4, 2)
    order = 4 * (at_row // 8) + lax.rem(at_row, 4)
    swapped = jnp.where(k_me == 0, 0, h_me)
    plain = lax.rem(1 - order // HALF + swapped, 2)
    origin = jnp.where((k_me == 0) & (h_me == 0), 2 * HALF, 2 * HALF - 1)
    inside = lax.rem(order, HALF)
    target = jnp.where(plain == 1, inside, HALF + lax.rem(origin - inside, HALF))
    target = target + which * LANES
    table[...] = jnp.where(target == at_column, 1.0, 0.0)

    def bins_turn(k, carry):
        block = bins_in[:, k].reshape(2 * LANES, LANES).astype(BF16)
        out = lax.dot_general(
            block, table[...].astype(BF16), (((0,), (0,)), ((), ())),
            preferred_element_type=F32,
        )
        bands[2 * k] = out[:, :LANES]
        bands[2 * k + 1] = out[:, LANES:]
        return carry

    lax.fori_loop(0, fold // 2, bins_turn, 0)
    sums[...] = jnp.zeros_like(sums)

    def band_step(k, carry):
        flipped = jnp.dot(
            reverse_of(k), bands[lax.rem(fold - k, fold)].astype(BF16),
            preferred_element_type=F32,
        )
        band = jnp.where(lane < HALF, bands[k], flipped)
        energy = power[k]
        for b in range(NBINS):
            kept = jnp.where(band == float(b), energy, 0.0)
            sums[b] += jnp.sum(kept.reshape(LANES // TILE, TILE, LANES), axis=0)
        return carry

    lax.fori_loop(0, fold, band_step, 0)
    totals = jnp.sum(jnp.sum(sums[...], axis=1), axis=1, keepdims=True)
    diagonal = lax.broadcasted_iota(jnp.int32, (NBINS, LANES), 0) == lax.broadcasted_iota(
        jnp.int32, (NBINS, LANES), 1
    )
    line = jnp.sum(jnp.where(diagonal, totals, 0.0), axis=0, keepdims=True)
    sums_out[...] = jnp.broadcast_to(line, (TILE, LANES))
    sums_in[me] = jnp.broadcast_to(line, (TILE, LANES))

    def tell(step):
        dest = lax.rem(me + step, devices)
        return pltpu.make_async_remote_copy(
            sums_out, sums_in.at[me], sum_send.at[step], sum_recv.at[step],
            device_id=place(dest), device_id_type=MESH,
        )

    def told(step):
        source = lax.rem(me + devices - step, devices)
        return pltpu.make_async_remote_copy(
            sums_out, sums_in.at[source], sum_send.at[step], sum_recv.at[step],
            device_id=place(source), device_id_type=MESH,
        )

    def tell_step(step, carry):
        tell(step).start()
        return carry

    lax.fori_loop(1, devices, tell_step, 0)

    def got_step(step, carry):
        got(step).wait_recv()
        return carry

    lax.fori_loop(1, devices, got_step, 0)

    def back_step(k, carry):
        angle = (lane * k).astype(F32) * angle_unit
        c, s = jnp.cos(angle), jnp.sin(angle)
        cos, sin = back_base[:, :LANES], back_base[:, LANES:]
        table[:, :LANES] = cos * c - sin * s
        table[:, LANES:] = sin * c + cos * s

        @pl.when(k == 0)
        def _():
            table[...] = back_zero[...]

        left = [
            jnp.concatenate(
                [arrived[2 * k + h, :, part * LANES:(part + 1) * LANES] for h in range(2)], 1
            )
            for part in range(2)
        ]
        folded[k, :2 * LANES] = dot3(jnp.concatenate(left, 0), table[...])
        return carry

    lax.fori_loop(0, slots, back_step, 0)

    for part, out in enumerate((out_real, out_imag)):
        def back_tile(i, carry, part=part, out=out):
            take = pl.ds(pl.multiple_of(part * LANES + i * TILE, TILE), TILE)
            spec = [(folded[0, take, :LANES], None)]
            for k in range(1, slots):
                spec.append((folded[k, take, :LANES], folded[k, take, LANES:]))
            spec.append((folded[0, take, LANES:], None))
            put = pl.ds(pl.multiple_of(i * TILE, TILE), TILE)
            for b, value in enumerate(real_inverse(spec, fold)):
                out[put, b * LANES:(b + 1) * LANES] = value
            return carry

        lax.fori_loop(0, LANES // TILE, back_tile, 0)

    def told_step(step, carry):
        told(step).wait_recv()
        return carry

    lax.fori_loop(1, devices, told_step, 0)
    out_spectrum[...] = jnp.sum(sums_in[...], axis=0)

    def last_step(step, carry):
        give(step).wait_send()
        tell(step).wait_send()
        send_bins(step).wait_send()
        return carry

    lax.fori_loop(1, devices, last_step, 0)

    def sent_step(dest, carry):
        for owner in range(planes):
            if owner > 0:
                @pl.when(p < owner)
                def _():
                    up(dest, owner).wait_send()

            if owner < planes - 1:
                @pl.when(p > owner)
                def _():
                    down(dest, owner).wait_send()

        @pl.when(dest != r)
        def _():
            cross(dest).wait_send()

        return carry

    lax.fori_loop(0, rows, sent_step, 0)


def folded_device(density, lens_weight, spectrum_bin):
    rows, planes = lax.axis_size("rows"), lax.axis_size("planes")
    devices = rows * planes
    slab, length = density.shape[1:]
    fold, blocks, slots = devices, slab // LANES, devices // 2
    groups = LANES // fold
    bins = spectrum_bin.reshape(LANES, fold // 2, 2, groups, fold)
    bins = bins.transpose(4, 1, 2, 3, 0).reshape(fold, fold // 2, 2 * groups, LANES)
    bins = bins.astype(F32)
    row_base, row_zero = row_tables(fold)
    back_base, back_zero = back_tables(fold)
    vmem = pl.BlockSpec(memory_space=pltpu.VMEM)
    hbm = pl.BlockSpec(memory_space=pl.ANY)
    smem = pl.BlockSpec(memory_space=pltpu.SMEM)
    dma = pltpu.SemaphoreType.DMA
    chunk = (blocks, LANES, LANES)
    scratch = [
        pltpu.VMEM((2, min(64, slab), length), F32),
        pltpu.VMEM((slots, slab, 2 * LANES), F32),
        pltpu.VMEM((rows, planes) + chunk, F32),
        pltpu.VMEM((rows, planes - 1) + chunk, F32),
        pltpu.VMEM((rows, planes - 1) + chunk, F32),
        pltpu.VMEM((fold, LANES, LANES), F32),
        pltpu.VMEM((fold, LANES, LANES), F32),
        pltpu.VMEM((fold, LANES, 2 * LANES), F32),
        pltpu.VMEM((fold, LANES, LANES), F32),
        pltpu.VMEM((devices, LANES, 2 * LANES), F32),
        pltpu.VMEM((devices, fold // 2, 2 * groups, LANES), F32),
        pltpu.VMEM((fold, LANES, LANES), F32),
        pltpu.VMEM((NBINS, TILE, LANES), F32),
        pltpu.VMEM((TILE, LANES), F32),
        pltpu.VMEM((devices, TILE, LANES), F32),
        pltpu.VMEM((2 * LANES, 2 * LANES), F32),
        dma((2,)),
        dma((rows, planes - 1)), dma((rows, planes - 1)),
        dma((rows, planes - 1)), dma((rows, planes - 1)),
        dma((rows,)), dma((rows,)),
        dma((devices,)), dma((devices,)), dma,
        dma((devices,)), dma((devices,)),
        dma((devices,)), dma((devices,)),
    ]
    real, imag, spectrum = pl.pallas_call(
        functools.partial(shear_kernel, rows, planes, slab),
        out_shape=(
            jax.ShapeDtypeStruct((length // devices, length), F32),
            jax.ShapeDtypeStruct((length // devices, length), F32),
            jax.ShapeDtypeStruct((TILE, LANES), F32),
        ),
        in_specs=[hbm, smem, hbm] + [vmem] * 6,
        out_specs=(vmem, vmem, vmem),
        scratch_shapes=scratch,
        compiler_params=pltpu.CompilerParams(
            collective_id=0, has_side_effects=True, vmem_limit_bytes=67043328
        ),
        name="shear",
    )(
        density[0], lens_weight, bins,
        row_base, row_zero, back_base, back_zero, column_table(), turn_table(length),
    )
    return real, imag, spectrum[0, :NBINS]


def phase(left, right, length, orient):
    index = np.arange(left)[:, None] * np.arange(right)[None, :] % length
    return np.exp(orient * 2j * math.pi * index / length)


def as_blocks(table):
    rows = np.stack([table.real, -table.imag], -1), np.stack([table.imag, table.real], -1)
    return np.stack(rows, 1).astype(np.float32)


def lane_table(table):
    top = np.concatenate([table.real, table.imag], 1)
    bottom = np.concatenate([-table.imag, table.real], 1)
    return np.concatenate([top, bottom], 0).astype(np.float32)


def product(pattern, left, right):
    return jnp.einsum(pattern, left, right, precision=lax.Precision.HIGH)


def turn(real, imag, table):
    cos, sin = table.real.astype(np.float32), table.imag.astype(np.float32)
    return real * cos - imag * sin, real * sin + imag * cos


def centred(indices, length):
    return ((indices + length // 2) % length - length // 2).astype(jnp.float32)


def plane_sum(density, lens_weight):
    count = lax.axis_size("planes")
    here = lax.axis_index("planes")
    block = density.shape[1] // count
    half = block // 2

    def own(owner, part):
        start = (owner % count) * block + part * half
        piece = lax.dynamic_slice_in_dim(density, start, half, axis=1)
        return jnp.sum(piece * lens_weight[:, None, None], axis=0)

    ways = ((0, 1), (1, -1))
    held = [own(here - way + count, part) for part, way in ways]
    for step in range(count - 1):
        moved = [
            lax.ppermute(held[part], "planes", [(i, (i + way) % count) for i in range(count)])
            for part, way in ways
        ]
        held = [
            moved[part] + own(here - way * (2 + step) + 2 * count, part) for part, way in ways
        ]
    return jnp.concatenate(held, axis=0)


def on_device(density, lens_weight, spectrum_bin):
    length = density.shape[-1]
    devices = lax.axis_size("rows") * lax.axis_size("planes")
    narrow = length // devices
    me = lax.axis_index("rows") * lax.axis_size("planes") + lax.axis_index("planes")

    share = plane_sum(density, lens_weight)
    field = share.T.reshape(narrow, devices, narrow)
    first = phase(narrow, narrow, narrow, -1)
    real = product("kn,nqy->kqy", first.real.astype(np.float32), field)
    imag = product("kn,nqy->kqy", first.imag.astype(np.float32), field)
    real, imag = turn(real, imag, phase(narrow, devices, length, -1)[:, :, None])
    forward = as_blocks(phase(devices, devices, devices, -1))
    spread = product("leq,kqy->leky", forward[..., 0], real) + product(
        "leq,kqy->leky", forward[..., 1], imag
    )
    held = lax.all_to_all(spread, AXES, split_axis=0, concat_axis=0, tiled=True)

    held = product("kesc,scxt->kext", forward, held)
    real, imag = turn(held[:, 0], held[:, 1], phase(devices, narrow, length, -1)[:, None, :])
    hat = product(
        "kxt,tm->kxm",
        jnp.concatenate([real, imag], -1),
        lane_table(phase(narrow, narrow, narrow, -1)),
    )
    hat_real, hat_imag = hat[..., :narrow], hat[..., narrow:]

    ky_index = (
        jnp.arange(devices, dtype=jnp.int32)[:, None, None]
        + devices * jnp.arange(narrow, dtype=jnp.int32)[None, None, :]
    )
    height = centred(ky_index, length)
    across = centred(me * narrow + jnp.arange(narrow, dtype=jnp.int32), length)[None, :, None]
    square_norm = height**2 + across**2
    anchor = square_norm == 0
    safe_norm = jnp.where(anchor, 1.0, square_norm)
    hat_real = jnp.where(anchor, 0.0, hat_real)
    hat_imag = jnp.where(anchor, 0.0, hat_imag)

    kernel_real = (across**2 - height**2) / safe_norm
    kernel_imag = 2.0 * across * height / safe_norm
    shear = jnp.concatenate(
        [
            kernel_real * hat_real - kernel_imag * hat_imag,
            kernel_real * hat_imag + kernel_imag * hat_real,
        ],
        -1,
    )
    back = product(
        "kxm,mt->kxt", shear, lane_table(phase(narrow, narrow, narrow, 1) / length)
    )
    real, imag = turn(
        back[..., :narrow], back[..., narrow:], phase(devices, narrow, length, 1)[:, None, :]
    )
    inverse = as_blocks(phase(devices, devices, devices, 1))
    back = product("sek,kxt->sext", inverse[..., 0], real) + product(
        "sek,kxt->sext", inverse[..., 1], imag
    )
    turned = lax.all_to_all(back, AXES, split_axis=0, concat_axis=0, tiled=True)

    pixel_power = (hat_real**2 + hat_imag**2) * (NBINS / float(length) ** 4)
    bins = spectrum_bin.reshape(narrow, devices, narrow).transpose(1, 2, 0)
    band_ids = jnp.arange(NBINS, dtype=jnp.int32)[:, None, None, None]
    partial_power = jnp.sum(jnp.where(bins == band_ids, pixel_power, 0.0), axis=(1, 2, 3))
    copies = jnp.broadcast_to(partial_power, (devices, 8, NBINS))
    gathered = lax.all_to_all(copies, AXES, split_axis=0, concat_axis=0, tiled=True)
    spectrum = jnp.sum(gathered[:, 0, :], axis=0)

    turned = product("aedc,dcqt->aeqt", inverse, turned)
    real, imag = turn(
        turned[:, 0], turned[:, 1], phase(devices, narrow, length, 1)[:, :, None]
    )
    last = phase(narrow, narrow, narrow, 1) / length
    cos, sin = last.real.astype(np.float32), last.imag.astype(np.float32)
    out_real = product("bq,aqt->bat", cos, real) - product("bq,aqt->bat", sin, imag)
    out_imag = product("bq,aqt->bat", sin, real) + product("bq,aqt->bat", cos, imag)
    shape = (length, narrow)
    return (out_real.reshape(shape).T, out_imag.reshape(shape).T, spectrum)


def folds(mesh, density):
    rows, planes = mesh.shape["rows"], mesh.shape["planes"]
    count, length, width = density.shape
    return (
        count == planes
        and planes % 2 == 0
        and planes >= 2
        and length == width == LANES * rows * planes
        and rows * planes == LANES // 4
    )


def solution(mesh):
    specs = (P("planes", "rows", None), P("planes"), P(None, AXES))
    outs = (P(AXES, None), P(AXES, None), P())

    def run(density, lens_weight, spectrum_bin):
        if folds(mesh, density):
            body = folded_device
        else:
            body = on_device
        whole = jax.shard_map(body, mesh=mesh, in_specs=specs, out_specs=outs, check_vma=False)
        return whole(density, lens_weight, spectrum_bin)

    return run
```

```python
import functools
import math

import jax
import jax.numpy as jnp
import numpy as np
from jax import lax
from jax.experimental import pallas as pl
from jax.experimental.pallas import tpu as pltpu
from jax.sharding import PartitionSpec as P

NBINS = 64
AXES = ("rows", "planes")
LANES = 128
HALF = LANES // 2
TILE = 8
MESH = pl.DeviceIdType.MESH
F32 = jnp.float32
BF16 = jnp.bfloat16


def real_fft(xs):
    n = len(xs)
    if n == 2:
        return [(xs[0] + xs[1], None), (xs[0] - xs[1], None)]
    even, odd = real_fft(xs[0::2]), real_fft(xs[1::2])
    out = [None] * (n // 2 + 1)
    out[0] = (even[0][0] + odd[0][0], None)
    out[n // 2] = (even[0][0] - odd[0][0], None)
    out[n // 4] = (even[n // 4][0], -odd[n // 4][0])
    for k in range(1, n // 4):
        c, s = math.cos(2 * math.pi * k / n), math.sin(2 * math.pi * k / n)
        (er, ei), (odr, odi) = even[k], odd[k]
        tr, ti = c * odr + s * odi, c * odi - s * odr
        out[k] = (er + tr, ei + ti)
        out[n // 2 - k] = (er - tr, ti - ei)
    return out


def real_inverse(spec, n):
    if n == 2:
        return [spec[0][0] + spec[1][0], spec[0][0] - spec[1][0]]
    h, q = n // 2, n // 4
    even, odd = [None] * (q + 1), [None] * (q + 1)
    even[0] = (spec[0][0] + spec[h][0], None)
    odd[0] = (spec[0][0] - spec[h][0], None)
    even[q] = (2.0 * spec[q][0], None)
    odd[q] = (-2.0 * spec[q][1], None)
    for k in range(1, q):
        (ar, ai), (br, bi) = spec[k], spec[h - k]
        even[k] = (ar + br, ai - bi)
        ur, ui = ar - br, ai + bi
        c, s = math.cos(2 * math.pi * k / n), math.sin(2 * math.pi * k / n)
        odd[k] = (c * ur - s * ui, c * ui + s * ur)
    evens, odds = real_inverse(even, h), real_inverse(odd, h)
    out = [None] * n
    out[0::2], out[1::2] = evens, odds
    return out


def packed_fft(xs, orient, swap, sign):
    n = len(xs)
    if n == 1:
        return xs
    even = packed_fft(xs[0::2], orient, swap, sign)
    odd = packed_fft(xs[1::2], orient, swap, sign)
    out = [None] * n
    for k in range(n // 2):
        c, s = math.cos(2 * math.pi * k / n), orient * math.sin(2 * math.pi * k / n)
        if k == 0:
            t = odd[0]
        elif 4 * k == n:
            t = swap(odd[k]) * (orient * sign)
        else:
            t = c * odd[k] + swap(odd[k]) * (s * sign)
        out[k], out[k + n // 2] = even[k] + t, even[k] - t
    return out


def split(x):
    high = x.astype(BF16)
    return high, (x - high.astype(F32)).astype(BF16)


def dot3(left, right):
    lh, ll = split(left)
    rh, rl = split(right)
    return jnp.dot(
        jnp.concatenate([lh, lh, ll], 1),
        jnp.concatenate([rh, rl, rh], 0),
        preferred_element_type=F32,
    )


def row_tables(fold):
    length = fold * LANES
    a = np.arange(LANES)
    general = np.zeros((2, LANES, 2, 2, HALF))
    special = np.zeros((2, LANES, 2, 2, HALF))
    for h in range(2):
        m = h * HALF + np.arange(HALF)
        angle = 2 * np.pi * (a[:, None] * m[None, :] % LANES) / LANES
        general[0, :, h, 0], general[0, :, h, 1] = np.cos(angle), -np.sin(angle)
        general[1, :, h, 0], general[1, :, h, 1] = np.sin(angle), np.cos(angle)
        kx = fold * np.arange(HALF) + h * (fold // 2)
        angle = 2 * np.pi * (a[:, None] * kx[None, :] % length) / length
        special[h, :, h, 0], special[h, :, h, 1] = np.cos(angle), -np.sin(angle)
    special[0, :, 0, 1, 0] = 1 - 2 * (a % 2)
    shape = (2 * LANES, 2 * LANES)
    return general.reshape(shape).astype(np.float32), special.reshape(shape).astype(np.float32)


def back_tables(fold):
    length = fold * LANES
    a = np.arange(LANES)
    general = np.zeros((2, 2, HALF, 2, LANES))
    special = np.zeros((2, 2, HALF, 2, LANES))
    for h in range(2):
        m = h * HALF + np.arange(HALF)
        angle = 2 * np.pi * (m[:, None] * a[None, :] % LANES) / LANES
        general[h, 0, :, 0], general[h, 0, :, 1] = np.cos(angle), np.sin(angle)
        general[h, 1, :, 0], general[h, 1, :, 1] = -np.sin(angle), np.cos(angle)
        kx = fold * np.arange(HALF) + h * (fold // 2)
        angle = 2 * np.pi * (kx[:, None] * a[None, :] % length) / length
        special[h, 0, :, h], special[h, 1, :, h] = 2 * np.cos(angle), -2 * np.sin(angle)
    special[0, 0, 0, 0] = 1.0
    special[0, 1, 0, 0] = 1 - 2 * (a % 2)
    shape, scale = (2 * LANES, 2 * LANES), float(length) ** -2
    return (
        (general.reshape(shape) * scale).astype(np.float32),
        (special.reshape(shape) * scale).astype(np.float32),
    )


def column_table():
    a = np.arange(LANES)
    angle = 2 * np.pi * (a[:, None] * a[None, :] % LANES) / LANES
    return np.concatenate([np.cos(angle), np.sin(angle)], 1).astype(np.float32)


def turn_table(length):
    angle = 2 * np.pi * np.arange(LANES)[:, None] / length * np.ones((1, LANES))
    return np.stack([np.cos(angle), np.sin(angle)]).astype(np.float32)


def shear_kernel(
    rows, planes, slab,
    density, weight, bins, row_base, row_zero, back_base, back_zero, column, turns,
    out_real, out_imag, out_spectrum,
    staged, folded, parts, far_low, far_high, near_low, near_high, lines, hat, shear, power,
    arrived, bins_raw, bins_out, bins_in, bands, sums, sums_out, sums_in, table, split_column,
    stage_sem, sum_send, sum_recv, cross_send, cross_recv,
    bins_send, bins_recv, bins_load, turn_send, turn_recv, total_send, total_recv,
):
    devices = rows * planes
    fold = devices
    length = fold * LANES
    slots = fold // 2
    blocks = slab // LANES
    middle = blocks // 2
    pairs = planes // 2
    angle_unit = 2 * math.pi / length
    r, p = lax.axis_index("rows"), lax.axis_index("planes")
    me = r * planes + p

    def place(device):
        return {"rows": device // planes, "planes": lax.rem(device, planes)}

    def remote(source, target, send, recv, device):
        return pltpu.make_async_remote_copy(
            source, target, send, recv, device_id=place(device), device_id_type=MESH
        )

    lane = lax.broadcasted_iota(jnp.int32, (1, LANES), 1)
    sign = jnp.where(lane < HALF, -1.0, 1.0)

    def swap(x):
        return pltpu.roll(x, HALF, axis=1)

    def times_i(x):
        return swap(x) * sign

    def minus_i(x):
        return swap(x) * (-sign)

    barrier = pltpu.get_barrier_semaphore()
    for step in range(1, devices):
        pl.semaphore_signal(
            barrier, inc=1, device_id=place(lax.rem(me + step, devices)), device_id_type=MESH
        )
    load_bins = pltpu.make_async_copy(bins, bins_raw, bins_load)
    load_bins.start()

    depth = staged.shape[1]
    chunks = slab // depth

    def stage(c):
        slot = lax.rem(c, 2)
        return pltpu.make_async_copy(
            density.at[pl.ds(c * depth, depth)], staged.at[slot], stage_sem.at[slot]
        )

    stage(0).start()
    scale = weight[0]

    def stage_step(c, carry):
        @pl.when(c + 1 < chunks)
        def _():
            stage(c + 1).start()

        stage(c).wait()
        slot = lax.rem(c, 2)

        def tile(i, carry):
            take = pl.ds(pl.multiple_of(i * TILE, TILE), TILE)
            xs = [staged[slot, take, b * LANES:(b + 1) * LANES] * scale for b in range(fold)]
            spec = real_fft(xs)
            put = pl.ds(pl.multiple_of(c * depth + i * TILE, TILE), TILE)
            folded[0, put, :LANES] = spec[0][0]
            folded[0, put, LANES:] = spec[slots][0]
            for k in range(1, slots):
                folded[k, put, :LANES] = spec[k][0]
                folded[k, put, LANES:] = spec[k][1]
            return carry

        return lax.fori_loop(0, depth // TILE, tile, carry)

    lax.fori_loop(0, chunks, stage_step, 0)
    pl.semaphore_wait(barrier, devices - 1)

    first, second = pl.ds(0, middle), pl.ds(middle, blocks - middle)
    above, below = lax.rem(p + 1, planes), lax.rem(p + planes - 1, planes)
    across_ring = lax.rem(p + 2, planes)

    def sum_copy(which, dest):
        owner, half, target, to = (
            (across_ring, first, far_high.at[dest], below),
            (across_ring, second, far_low.at[dest], above),
            (above, first, near_low.at[dest, first], above),
            (above, second, near_low.at[dest, second], above),
            (below, first, near_high.at[dest, first], below),
            (below, second, near_high.at[dest, second], below),
        )[which]
        return remote(
            parts.at[dest, owner, half], target,
            sum_send.at[which, dest], sum_recv.at[which, dest], r * planes + to,
        )

    def cross(dest):
        return remote(
            parts.at[dest, p], lines.at[pl.ds(r * blocks, blocks)],
            cross_send.at[dest], cross_recv.at[r], dest * planes + p,
        )

    def crossed(source):
        return remote(
            parts.at[source, p], lines.at[pl.ds(source * blocks, blocks)],
            cross_send.at[source], cross_recv.at[source], source * planes + p,
        )

    at_a = lax.broadcasted_iota(jnp.int32, (LANES, LANES), 0)

    def row_step(i, carry):
        dest = lax.rem(r + 1 + i, rows)
        for pair in range(pairs):
            k = dest * pairs + pair
            angle = (at_a * k).astype(F32) * angle_unit
            c, s = jnp.cos(angle), jnp.sin(angle)
            c, s = jnp.concatenate([c, c], 1), jnp.concatenate([s, s], 1)
            top, low = row_base[:LANES], row_base[LANES:]
            table[:LANES] = c * top - s * low
            table[LANES:] = c * low + s * top

            @pl.when(k == 0)
            def _():
                table[...] = row_zero[...]

            right = table[...]
            for q in range(blocks):
                done = dot3(folded[k, q * LANES:(q + 1) * LANES], right)
                parts[dest, 2 * pair, q] = done[:, :LANES]
                parts[dest, 2 * pair + 1, q] = done[:, LANES:]

        for which in (0, 1, 2, 5):
            sum_copy(which, dest).start()
        return carry

    lax.fori_loop(0, rows, row_step, 0)

    at_row = lax.broadcasted_iota(jnp.int32, (2 * LANES, 2 * LANES), 0)
    at_column = lax.broadcasted_iota(jnp.int32, (2 * LANES, 2 * LANES), 1)
    which_row = lax.rem(at_row // 4, 2)
    target = which_row * LANES + lax.rem(at_row, 4) * fold + at_row // 8
    table[...] = jnp.where(target == at_column, 1.0, 0.0)
    load_bins.wait()

    def bins_layout(k, carry):
        both = [bins_raw[pl.ds(2 * k + q, LANES, stride=fold), :] for q in range(2)]
        both = jnp.concatenate(both, 1).astype(F32).astype(BF16)
        out = lax.dot_general(
            table[...].astype(BF16), both, (((1,), (1,)), ((), ())), preferred_element_type=F32
        )
        bins_out[:, k] = out.reshape(fold, TILE, LANES)
        return carry

    lax.fori_loop(0, fold // 2, bins_layout, 0)
    side = me // slots

    def class_at(owner):
        k, h = owner // 2, lax.rem(owner, 2)
        other = k + lax.rem(h + side, 2) * (fold - 2 * k)
        return jnp.where(k == 0, h * slots, other)

    def send_bins(step):
        owner = lax.rem(me + step, devices)
        return remote(
            bins_out.at[class_at(owner)], bins_in.at[me],
            bins_send.at[step], bins_recv.at[step], owner,
        )

    def recv_bins(step):
        source = lax.rem(me + devices - step, devices)
        return remote(
            bins_out.at[0], bins_in.at[source], bins_send.at[step], bins_recv.at[step], source
        )

    def relay_step(i, carry):
        dest = lax.rem(r + 1 + i, rows)
        sum_copy(1, dest).wait_recv()
        parts[dest, above, second] = parts[dest, above, second] + far_low[dest]
        sum_copy(3, dest).start()
        sum_copy(0, dest).wait_recv()
        parts[dest, below, first] = parts[dest, below, first] + far_high[dest]
        sum_copy(4, dest).start()
        return carry

    lax.fori_loop(0, rows, relay_step, 0)

    def bins_step(step, carry):
        send_bins(step).start()
        return carry

    lax.fori_loop(1, devices, bins_step, 0)
    bins_in[me] = bins_out[class_at(me)]

    def owner_step(i, carry):
        dest = lax.rem(r + 1 + i, rows)
        for which in (2, 3, 4, 5):
            sum_copy(which, dest).wait_recv()
        parts[dest, p] = parts[dest, p] + near_low[dest] + near_high[dest]

        @pl.when(dest != r)
        def _():
            cross(dest).start()

        return carry

    lax.fori_loop(0, rows, owner_step, 0)

    def own_step(q, carry):
        lines[r * blocks + q] = parts[r, p, q]
        return carry

    lax.fori_loop(0, blocks, own_step, 0)

    def crossed_step(i, carry):
        crossed(lax.rem(r + rows - 1 - i, rows)).wait_recv()
        return carry

    lax.fori_loop(0, rows - 1, crossed_step, 0)

    def column_tile(i, carry):
        take = pl.ds(pl.multiple_of(i * TILE, TILE), TILE)
        spec = packed_fft([lines[b, take] for b in range(fold)], -1, swap, sign)
        lines[0, take] = spec[0]
        c1, s1 = turns[0, take], turns[1, take] * sign
        c, s = c1, s1
        for k in range(1, fold):
            lines[k, take] = spec[k] * c - swap(spec[k]) * s
            c, s = c * c1 - s * s1, s * c1 + c * s1
        return carry

    lax.fori_loop(0, LANES // TILE, column_tile, 0)

    k_me, h_me = me // 2, lax.rem(me, 2)
    index = lax.rem(lane, HALF)
    kx = jnp.where(
        k_me == 0, fold * index + h_me * slots, fold * (HALF * h_me + index) + k_me
    )
    across = jnp.where(kx >= length // 2, kx - length, kx).astype(F32)
    my = lax.broadcasted_iota(jnp.int32, (LANES, LANES), 0)
    at_lane = lax.broadcasted_iota(jnp.int32, (LANES, LANES), 1)
    pixel_scale = NBINS / float(length) ** 4

    def height_of(k):
        ky = k + fold * my
        return jnp.where(ky >= length // 2, ky - length, ky).astype(F32)

    def kernel_of(width, height):
        square_norm = height * height + width * width
        safe = jnp.where(square_norm == 0.0, 1.0, square_norm)
        inverse = 1.0 / safe
        return (width * width - height * height) * inverse, 2.0 * width * height * inverse

    def edge_of(k):
        return (my == HALF) & (k == 0)

    high, low = split(column[...])
    split_column[...] = jnp.concatenate([high, high, low], 1)

    def column_product(right):
        rh, rl = split(right)
        return jnp.dot(
            split_column[...], jnp.concatenate([rh, rl, rh], 0), preferred_element_type=F32
        )

    def each(f, x):
        count = x.shape[1] // LANES
        return jnp.concatenate([f(x[:, q * LANES:(q + 1) * LANES]) for q in range(count)], 1)

    def column_step(j, carry):
        z = jnp.concatenate([lines[2 * j], lines[2 * j + 1]], 1)
        both = column_product(jnp.concatenate([z, each(minus_i, z)], 0))
        turned = []
        for q in range(2):
            k = 2 * j + q
            v = both[:, q * LANES:(q + 1) * LANES]
            hat[k] = v
            square = v * v
            power[k] = (square + swap(square)) * pixel_scale
            kernel_real, kernel_imag = kernel_of(across, height_of(k))
            edge = edge_of(k)
            turned += [
                kernel_real * v + jnp.where(edge, kernel_imag * times_i(v), 0.0),
                jnp.where(edge, 0.0, kernel_imag * v),
            ]
        turned = jnp.concatenate(turned, 1)
        back = column_product(jnp.concatenate([turned, each(times_i, turned)], 0))
        shear[2 * j] = back[:, :2 * LANES]
        shear[2 * j + 1] = back[:, 2 * LANES:]
        return carry

    lax.fori_loop(0, fold // 2, column_step, 0)

    def reverse_of(wrap):
        return jnp.where(lax.rem(LANES - wrap - my, LANES) == at_lane, 1.0, 0.0).astype(BF16)

    @pl.when(me == 0)
    def _():
        spot = lax.rem(at_lane, HALF)

        def gather(k, held):
            return jnp.where(spot == k, pltpu.roll(hat[k], k, axis=1), held)

        v = lax.fori_loop(0, fold, gather, jnp.zeros((LANES, LANES), F32))
        high, low = split(v)

        def moved(wrap):
            mover = reverse_of(wrap)
            return jnp.dot(mover, high, preferred_element_type=F32) + jnp.dot(
                mover, low, preferred_element_type=F32
            )

        my_spot = lax.rem(my, HALF)
        same = (my // HALF == at_lane // HALF) & (spot < fold)
        partner = jnp.where(same & (lax.rem(fold - spot, fold) == my_spot), 1.0, 0.0)
        partner = partner.astype(BF16)
        high, low = split(jnp.where(spot == 0, moved(0), moved(1)))
        mirror = jnp.dot(high, partner, preferred_element_type=F32) + jnp.dot(
            low, partner, preferred_element_type=F32
        )
        mirror = mirror * (-sign)
        zero = jnp.where((my == 0) & (spot == 0), 0.0, (v + mirror) * 0.5)
        last = minus_i((v - mirror) * 0.5)
        zero_square, last_square = zero * zero, last * last
        powers = jnp.where(
            at_lane < HALF, zero_square + swap(zero_square), last_square + swap(last_square)
        ) * pixel_scale
        ky = spot + fold * my
        height = jnp.where(ky >= length // 2, ky - length, ky).astype(F32)
        kernel_real, kernel_imag = kernel_of(float(-(length // 2)), height)
        turned = times_i(kernel_real * last + kernel_imag * times_i(last))
        edge = ky == length // 2
        real = jnp.where(edge, 0.0, turned) - zero
        imag = jnp.where(edge, times_i(last), 0.0)
        both = jnp.concatenate([real, imag], 1)
        back = column_product(jnp.concatenate([both, each(times_i, both)], 0))

        def scatter(k, carry):
            shift = lax.rem(LANES - k, LANES)
            for part in range(2):
                span = slice(part * LANES, (part + 1) * LANES)
                value = pltpu.roll(back[:, span], shift, axis=1)
                shear[k, :, span] = jnp.where(spot == 0, value, shear[k, :, span])
            power[k] = jnp.where(spot == 0, pltpu.roll(powers, shift, axis=1), power[k])
            return carry

        lax.fori_loop(0, fold, scatter, 0)

    def inverse_tile(i, carry):
        take = pl.ds(pl.multiple_of(i * TILE, TILE), TILE)
        c1, s1 = turns[0, take], turns[1, take] * sign
        for part in range(2):
            span = slice(part * LANES, (part + 1) * LANES)
            c, s = c1, s1
            held = [shear[0, take, span]]
            for k in range(1, fold):
                value = shear[k, take, span]
                held.append(value * c + swap(value) * s)
                c, s = c * c1 - s * s1, s * c1 + c * s1
            for b, value in enumerate(packed_fft(held, 1, swap, sign)):
                shear[b, take, span] = value
        return carry

    lax.fori_loop(0, LANES // TILE, inverse_tile, 0)

    def give(dest):
        return remote(
            shear.at[dest], arrived.at[me], turn_send.at[dest], turn_recv.at[me], dest
        )

    def got(source):
        return remote(
            shear.at[source], arrived.at[source], turn_send.at[source], turn_recv.at[source],
            source,
        )

    for turn in (2, 1, 3, 0):
        def give_step(i, carry, turn=turn):
            dest = lax.rem(r + i, rows) * planes + lax.rem(p + turn, planes)
            give(dest).start()
            return carry

        lax.fori_loop(1 if turn == 0 else 0, rows, give_step, 0)
    arrived[me] = shear[me]

    def bins_wait(step, carry):
        recv_bins(step).wait_recv()
        return carry

    lax.fori_loop(1, devices, bins_wait, 0)

    order = 4 * (at_row // 8) + lax.rem(at_row, 4)
    swapped = jnp.where(k_me == 0, 0, h_me)
    plain = lax.rem(1 - order // HALF + swapped, 2)
    origin = jnp.where((k_me == 0) & (h_me == 0), 2 * HALF, 2 * HALF - 1)
    inside = lax.rem(order, HALF)
    target = jnp.where(plain == 1, inside, HALF + lax.rem(origin - inside, HALF))
    target = target + which_row * LANES
    table[...] = jnp.where(target == at_column, 1.0, 0.0)

    def bins_turn(k, carry):
        block = bins_in[:, k].reshape(2 * LANES, LANES).astype(BF16)
        out = lax.dot_general(
            block, table[...].astype(BF16), (((0,), (0,)), ((), ())),
            preferred_element_type=F32,
        )
        bands[2 * k] = out[:, :LANES]
        bands[2 * k + 1] = out[:, LANES:]
        return carry

    lax.fori_loop(0, fold // 2, bins_turn, 0)
    sums[...] = jnp.zeros_like(sums)

    def band_step(k, carry):
        flipped = jnp.dot(
            reverse_of(jnp.where(k == 0, 0, 1)), bands[lax.rem(fold - k, fold)].astype(BF16),
            preferred_element_type=F32,
        )
        band = jnp.where(lane < HALF, bands[k], flipped)
        energy = power[k]
        for b in range(NBINS):
            kept = jnp.where(band == float(b), energy, 0.0)
            sums[b] += jnp.sum(kept.reshape(LANES // TILE, TILE, LANES), axis=0)
        return carry

    lax.fori_loop(0, fold, band_step, 0)
    totals = jnp.sum(jnp.sum(sums[...], axis=1), axis=1, keepdims=True)
    diagonal = lax.broadcasted_iota(jnp.int32, (NBINS, LANES), 0) == lax.broadcasted_iota(
        jnp.int32, (NBINS, LANES), 1
    )
    line = jnp.sum(jnp.where(diagonal, totals, 0.0), axis=0, keepdims=True)
    sums_out[...] = jnp.broadcast_to(line, (TILE, LANES))
    sums_in[me] = jnp.broadcast_to(line, (TILE, LANES))

    def tell(step):
        dest = lax.rem(me + step, devices)
        return remote(sums_out, sums_in.at[me], total_send.at[step], total_recv.at[step], dest)

    def told(step):
        source = lax.rem(me + devices - step, devices)
        return remote(
            sums_out, sums_in.at[source], total_send.at[step], total_recv.at[step], source
        )

    def tell_step(step, carry):
        tell(step).start()
        return carry

    lax.fori_loop(1, devices, tell_step, 0)

    def back_step(i, carry):
        k = lax.rem(me // 2 + slots - i, slots)
        for h in range(2):
            @pl.when(2 * k + h != me)
            def _():
                got(2 * k + h).wait_recv()

        angle = (lane * k).astype(F32) * angle_unit
        c, s = jnp.cos(angle), jnp.sin(angle)
        cos, sin = back_base[:, :LANES], back_base[:, LANES:]
        table[:, :LANES] = cos * c - sin * s
        table[:, LANES:] = sin * c + cos * s

        @pl.when(k == 0)
        def _():
            table[...] = back_zero[...]

        left = [
            jnp.concatenate(
                [arrived[2 * k + h, :, part * LANES:(part + 1) * LANES] for h in range(2)], 1
            )
            for part in range(2)
        ]
        folded[k, :2 * LANES] = dot3(jnp.concatenate(left, 0), table[...])
        return carry

    lax.fori_loop(0, slots, back_step, 0)

    for part, out in enumerate((out_real, out_imag)):
        def back_tile(i, carry, part=part, out=out):
            take = pl.ds(pl.multiple_of(part * LANES + i * TILE, TILE), TILE)
            spec = [(folded[0, take, :LANES], None)]
            for k in range(1, slots):
                spec.append((folded[k, take, :LANES], folded[k, take, LANES:]))
            spec.append((folded[0, take, LANES:], None))
            put = pl.ds(pl.multiple_of(i * TILE, TILE), TILE)
            for b, value in enumerate(real_inverse(spec, fold)):
                out[put, b * LANES:(b + 1) * LANES] = value
            return carry

        lax.fori_loop(0, LANES // TILE, back_tile, 0)

    def told_step(step, carry):
        told(step).wait_recv()
        return carry

    lax.fori_loop(1, devices, told_step, 0)
    out_spectrum[...] = jnp.sum(sums_in[...], axis=0)

    def last_step(step, carry):
        give(lax.rem(me + step, devices)).wait_send()
        tell(step).wait_send()
        send_bins(step).wait_send()
        return carry

    lax.fori_loop(1, devices, last_step, 0)

    def sent_step(dest, carry):
        for which in range(6):
            sum_copy(which, dest).wait_send()

        @pl.when(dest != r)
        def _():
            cross(dest).wait_send()

        return carry

    lax.fori_loop(0, rows, sent_step, 0)


def folded_device(density, lens_weight, spectrum_bin):
    rows, planes = lax.axis_size("rows"), lax.axis_size("planes")
    devices = rows * planes
    slab, length = density.shape[1:]
    fold, blocks, slots = devices, slab // LANES, devices // 2
    middle = blocks // 2
    row_base, row_zero = row_tables(fold)
    back_base, back_zero = back_tables(fold)
    vmem = pl.BlockSpec(memory_space=pltpu.VMEM)
    hbm = pl.BlockSpec(memory_space=pl.ANY)
    smem = pl.BlockSpec(memory_space=pltpu.SMEM)
    dma = pltpu.SemaphoreType.DMA
    chunk = (blocks, LANES, LANES)
    scratch = [
        pltpu.VMEM((2, min(64, slab), length), F32),
        pltpu.VMEM((slots, slab, 2 * LANES), F32),
        pltpu.VMEM((rows, planes) + chunk, F32),
        pltpu.VMEM((rows, blocks - middle, LANES, LANES), F32),
        pltpu.VMEM((rows, middle, LANES, LANES), F32),
        pltpu.VMEM((rows,) + chunk, F32),
        pltpu.VMEM((rows,) + chunk, F32),
        pltpu.VMEM((fold, LANES, LANES), F32),
        pltpu.VMEM((fold, LANES, LANES), F32),
        pltpu.VMEM((fold, LANES, 2 * LANES), F32),
        pltpu.VMEM((fold, LANES, LANES), F32),
        pltpu.VMEM((devices, LANES, 2 * LANES), F32),
        pltpu.VMEM((length, LANES), jnp.int32),
        pltpu.VMEM((fold, fold // 2, TILE, LANES), F32),
        pltpu.VMEM((devices, fold // 2, TILE, LANES), F32),
        pltpu.VMEM((fold, LANES, LANES), F32),
        pltpu.VMEM((NBINS, TILE, LANES), F32),
        pltpu.VMEM((TILE, LANES), F32),
        pltpu.VMEM((devices, TILE, LANES), F32),
        pltpu.VMEM((2 * LANES, 2 * LANES), F32),
        pltpu.VMEM((LANES, 6 * LANES), BF16),
        dma((2,)),
        dma((6, rows)), dma((6, rows)),
        dma((rows,)), dma((rows,)),
        dma((devices,)), dma((devices,)), dma,
        dma((devices,)), dma((devices,)),
        dma((devices,)), dma((devices,)),
    ]
    real, imag, spectrum = pl.pallas_call(
        functools.partial(shear_kernel, rows, planes, slab),
        out_shape=(
            jax.ShapeDtypeStruct((length // devices, length), F32),
            jax.ShapeDtypeStruct((length // devices, length), F32),
            jax.ShapeDtypeStruct((TILE, LANES), F32),
        ),
        in_specs=[hbm, smem, hbm] + [vmem] * 6,
        out_specs=(vmem, vmem, vmem),
        scratch_shapes=scratch,
        compiler_params=pltpu.CompilerParams(
            collective_id=0, has_side_effects=True, vmem_limit_bytes=67043328
        ),
        name="shear",
    )(
        density[0], lens_weight, spectrum_bin,
        row_base, row_zero, back_base, back_zero, column_table(), turn_table(length),
    )
    return real, imag, spectrum[0, :NBINS]


def phase(left, right, length, orient):
    index = np.arange(left)[:, None] * np.arange(right)[None, :] % length
    return np.exp(orient * 2j * math.pi * index / length)


def as_blocks(table):
    rows = np.stack([table.real, -table.imag], -1), np.stack([table.imag, table.real], -1)
    return np.stack(rows, 1).astype(np.float32)


def lane_table(table):
    top = np.concatenate([table.real, table.imag], 1)
    bottom = np.concatenate([-table.imag, table.real], 1)
    return np.concatenate([top, bottom], 0).astype(np.float32)


def product(pattern, left, right):
    return jnp.einsum(pattern, left, right, precision=lax.Precision.HIGH)


def turn(real, imag, table):
    cos, sin = table.real.astype(np.float32), table.imag.astype(np.float32)
    return real * cos - imag * sin, real * sin + imag * cos


def centred(indices, length):
    return ((indices + length // 2) % length - length // 2).astype(jnp.float32)


def plane_sum(density, lens_weight):
    count = lax.axis_size("planes")
    here = lax.axis_index("planes")
    block = density.shape[1] // count
    half = block // 2

    def own(owner, part):
        start = (owner % count) * block + part * half
        piece = lax.dynamic_slice_in_dim(density, start, half, axis=1)
        return jnp.sum(piece * lens_weight[:, None, None], axis=0)

    ways = ((0, 1), (1, -1))
    held = [own(here - way + count, part) for part, way in ways]
    for step in range(count - 1):
        moved = [
            lax.ppermute(held[part], "planes", [(i, (i + way) % count) for i in range(count)])
            for part, way in ways
        ]
        held = [
            moved[part] + own(here - way * (2 + step) + 2 * count, part) for part, way in ways
        ]
    return jnp.concatenate(held, axis=0)


def on_device(density, lens_weight, spectrum_bin):
    length = density.shape[-1]
    devices = lax.axis_size("rows") * lax.axis_size("planes")
    narrow = length // devices
    me = lax.axis_index("rows") * lax.axis_size("planes") + lax.axis_index("planes")

    share = plane_sum(density, lens_weight)
    field = share.T.reshape(narrow, devices, narrow)
    first = phase(narrow, narrow, narrow, -1)
    real = product("kn,nqy->kqy", first.real.astype(np.float32), field)
    imag = product("kn,nqy->kqy", first.imag.astype(np.float32), field)
    real, imag = turn(real, imag, phase(narrow, devices, length, -1)[:, :, None])
    forward = as_blocks(phase(devices, devices, devices, -1))
    spread = product("leq,kqy->leky", forward[..., 0], real) + product(
        "leq,kqy->leky", forward[..., 1], imag
    )
    held = lax.all_to_all(spread, AXES, split_axis=0, concat_axis=0, tiled=True)

    held = product("kesc,scxt->kext", forward, held)
    real, imag = turn(held[:, 0], held[:, 1], phase(devices, narrow, length, -1)[:, None, :])
    hat = product(
        "kxt,tm->kxm",
        jnp.concatenate([real, imag], -1),
        lane_table(phase(narrow, narrow, narrow, -1)),
    )
    hat_real, hat_imag = hat[..., :narrow], hat[..., narrow:]

    ky_index = (
        jnp.arange(devices, dtype=jnp.int32)[:, None, None]
        + devices * jnp.arange(narrow, dtype=jnp.int32)[None, None, :]
    )
    height = centred(ky_index, length)
    across = centred(me * narrow + jnp.arange(narrow, dtype=jnp.int32), length)[None, :, None]
    square_norm = height**2 + across**2
    anchor = square_norm == 0
    safe_norm = jnp.where(anchor, 1.0, square_norm)
    hat_real = jnp.where(anchor, 0.0, hat_real)
    hat_imag = jnp.where(anchor, 0.0, hat_imag)

    kernel_real = (across**2 - height**2) / safe_norm
    kernel_imag = 2.0 * across * height / safe_norm
    shear = jnp.concatenate(
        [
            kernel_real * hat_real - kernel_imag * hat_imag,
            kernel_real * hat_imag + kernel_imag * hat_real,
        ],
        -1,
    )
    back = product(
        "kxm,mt->kxt", shear, lane_table(phase(narrow, narrow, narrow, 1) / length)
    )
    real, imag = turn(
        back[..., :narrow], back[..., narrow:], phase(devices, narrow, length, 1)[:, None, :]
    )
    inverse = as_blocks(phase(devices, devices, devices, 1))
    back = product("sek,kxt->sext", inverse[..., 0], real) + product(
        "sek,kxt->sext", inverse[..., 1], imag
    )
    turned = lax.all_to_all(back, AXES, split_axis=0, concat_axis=0, tiled=True)

    pixel_power = (hat_real**2 + hat_imag**2) * (NBINS / float(length) ** 4)
    bins = spectrum_bin.reshape(narrow, devices, narrow).transpose(1, 2, 0)
    band_ids = jnp.arange(NBINS, dtype=jnp.int32)[:, None, None, None]
    partial_power = jnp.sum(jnp.where(bins == band_ids, pixel_power, 0.0), axis=(1, 2, 3))
    copies = jnp.broadcast_to(partial_power, (devices, 8, NBINS))
    gathered = lax.all_to_all(copies, AXES, split_axis=0, concat_axis=0, tiled=True)
    spectrum = jnp.sum(gathered[:, 0, :], axis=0)

    turned = product("aedc,dcqt->aeqt", inverse, turned)
    real, imag = turn(
        turned[:, 0], turned[:, 1], phase(devices, narrow, length, 1)[:, :, None]
    )
    last = phase(narrow, narrow, narrow, 1) / length
    cos, sin = last.real.astype(np.float32), last.imag.astype(np.float32)
    out_real = product("bq,aqt->bat", cos, real) - product("bq,aqt->bat", sin, imag)
    out_imag = product("bq,aqt->bat", sin, real) + product("bq,aqt->bat", cos, imag)
    shape = (length, narrow)
    return (out_real.reshape(shape).T, out_imag.reshape(shape).T, spectrum)


def folds(mesh, density):
    rows, planes = mesh.shape["rows"], mesh.shape["planes"]
    count, length, width = density.shape
    return (
        count == planes
        and planes == 4
        and length == width == LANES * rows * planes
        and rows * planes == LANES // 4
    )


def solution(mesh):
    specs = (P("planes", "rows", None), P("planes"), P(None, AXES))
    outs = (P(AXES, None), P(AXES, None), P())

    def run(density, lens_weight, spectrum_bin):
        if folds(mesh, density):
            body = folded_device
        else:
            body = on_device
        whole = jax.shard_map(body, mesh=mesh, in_specs=specs, out_specs=outs, check_vma=False)
        return whole(density, lens_weight, spectrum_bin)

    return run
```

```python
import functools
import math

import jax
import jax.numpy as jnp
import numpy as np
from jax import lax
from jax.experimental import pallas as pl
from jax.experimental.pallas import tpu as pltpu
from jax.sharding import PartitionSpec as P

NBINS = 64
AXES = ("rows", "planes")
LANES = 128
HALF = LANES // 2
TILE = 8
MESH = pl.DeviceIdType.MESH
F32 = jnp.float32
BF16 = jnp.bfloat16


def real_fft(xs):
    n = len(xs)
    if n == 2:
        return [(xs[0] + xs[1], None), (xs[0] - xs[1], None)]
    even, odd = real_fft(xs[0::2]), real_fft(xs[1::2])
    out = [None] * (n // 2 + 1)
    out[0] = (even[0][0] + odd[0][0], None)
    out[n // 2] = (even[0][0] - odd[0][0], None)
    out[n // 4] = (even[n // 4][0], -odd[n // 4][0])
    for k in range(1, n // 4):
        c, s = math.cos(2 * math.pi * k / n), math.sin(2 * math.pi * k / n)
        (er, ei), (odr, odi) = even[k], odd[k]
        tr, ti = c * odr + s * odi, c * odi - s * odr
        out[k] = (er + tr, ei + ti)
        out[n // 2 - k] = (er - tr, ti - ei)
    return out


def real_inverse(spec, n):
    if n == 2:
        return [spec[0][0] + spec[1][0], spec[0][0] - spec[1][0]]
    h, q = n // 2, n // 4
    even, odd = [None] * (q + 1), [None] * (q + 1)
    even[0] = (spec[0][0] + spec[h][0], None)
    odd[0] = (spec[0][0] - spec[h][0], None)
    even[q] = (2.0 * spec[q][0], None)
    odd[q] = (-2.0 * spec[q][1], None)
    for k in range(1, q):
        (ar, ai), (br, bi) = spec[k], spec[h - k]
        even[k] = (ar + br, ai - bi)
        ur, ui = ar - br, ai + bi
        c, s = math.cos(2 * math.pi * k / n), math.sin(2 * math.pi * k / n)
        odd[k] = (c * ur - s * ui, c * ui + s * ur)
    evens, odds = real_inverse(even, h), real_inverse(odd, h)
    out = [None] * n
    out[0::2], out[1::2] = evens, odds
    return out


def packed_fft(xs, orient, swap, sign):
    n = len(xs)
    if n == 1:
        return xs
    even = packed_fft(xs[0::2], orient, swap, sign)
    odd = packed_fft(xs[1::2], orient, swap, sign)
    out = [None] * n
    for k in range(n // 2):
        c, s = math.cos(2 * math.pi * k / n), orient * math.sin(2 * math.pi * k / n)
        if k == 0:
            t = odd[0]
        elif 4 * k == n:
            t = swap(odd[k]) * (orient * sign)
        else:
            t = c * odd[k] + swap(odd[k]) * (s * sign)
        out[k], out[k + n // 2] = even[k] + t, even[k] - t
    return out


def split(x):
    high = x.astype(BF16)
    return high, (x - high.astype(F32)).astype(BF16)


def dot3(left, right):
    lh, ll = split(left)
    rh, rl = split(right)
    return jnp.dot(
        jnp.concatenate([lh, lh, ll], 1),
        jnp.concatenate([rh, rl, rh], 0),
        preferred_element_type=F32,
    )


def row_tables(fold):
    length = fold * LANES
    a = np.arange(LANES)
    general = np.zeros((2, LANES, 2, 2, HALF))
    special = np.zeros((2, LANES, 2, 2, HALF))
    for h in range(2):
        m = h * HALF + np.arange(HALF)
        angle = 2 * np.pi * (a[:, None] * m[None, :] % LANES) / LANES
        general[0, :, h, 0], general[0, :, h, 1] = np.cos(angle), -np.sin(angle)
        general[1, :, h, 0], general[1, :, h, 1] = np.sin(angle), np.cos(angle)
        kx = fold * np.arange(HALF) + h * (fold // 2)
        angle = 2 * np.pi * (a[:, None] * kx[None, :] % length) / length
        special[h, :, h, 0], special[h, :, h, 1] = np.cos(angle), -np.sin(angle)
    special[0, :, 0, 1, 0] = 1 - 2 * (a % 2)
    shape = (2 * LANES, 2 * LANES)
    return general.reshape(shape).astype(np.float32), special.reshape(shape).astype(np.float32)


def back_tables(fold):
    length = fold * LANES
    a = np.arange(LANES)
    general = np.zeros((2, 2, HALF, 2, LANES))
    special = np.zeros((2, 2, HALF, 2, LANES))
    for h in range(2):
        m = h * HALF + np.arange(HALF)
        angle = 2 * np.pi * (m[:, None] * a[None, :] % LANES) / LANES
        general[h, 0, :, 0], general[h, 0, :, 1] = np.cos(angle), np.sin(angle)
        general[h, 1, :, 0], general[h, 1, :, 1] = -np.sin(angle), np.cos(angle)
        kx = fold * np.arange(HALF) + h * (fold // 2)
        angle = 2 * np.pi * (kx[:, None] * a[None, :] % length) / length
        special[h, 0, :, h], special[h, 1, :, h] = 2 * np.cos(angle), -2 * np.sin(angle)
    special[0, 0, 0, 0] = 1.0
    special[0, 1, 0, 0] = 1 - 2 * (a % 2)
    shape, scale = (2 * LANES, 2 * LANES), float(length) ** -2
    return (
        (general.reshape(shape) * scale).astype(np.float32),
        (special.reshape(shape) * scale).astype(np.float32),
    )


def column_table():
    a = np.arange(LANES)
    angle = 2 * np.pi * (a[:, None] * a[None, :] % LANES) / LANES
    return np.concatenate([np.cos(angle), np.sin(angle)], 1).astype(np.float32)


def turn_table(length):
    angle = 2 * np.pi * np.arange(LANES)[:, None] / length * np.ones((1, LANES))
    return np.stack([np.cos(angle), np.sin(angle)]).astype(np.float32)


def shear_kernel(
    rows, planes, slab,
    density, weight, bins, row_base, row_zero, back_base, back_zero, column, turns,
    out_real, out_imag, out_spectrum,
    staged, folded, parts, outer_inner, outer_own, outer_far, inner_outer, last_own, lines, hat, shear, power,
    arrived, bins_raw, bins_out, bins_in, bands, sums, sums_out, sums_in, table, split_column,
    stage_sem, sum_send, sum_recv, cross_send, cross_recv,
    bins_send, bins_recv, bins_load, turn_send, turn_recv, total_send, total_recv,
):
    devices = rows * planes
    fold = devices
    length = fold * LANES
    slots = fold // 2
    blocks = slab // LANES
    pairs = planes // 2
    angle_unit = 2 * math.pi / length
    r, p = lax.axis_index("rows"), lax.axis_index("planes")
    me = r * planes + p

    def place(device):
        return {"rows": device // planes, "planes": lax.rem(device, planes)}

    def remote(source, target, send, recv, device):
        return pltpu.make_async_remote_copy(
            source, target, send, recv, device_id=place(device), device_id_type=MESH
        )

    lane = lax.broadcasted_iota(jnp.int32, (1, LANES), 1)
    sign = jnp.where(lane < HALF, -1.0, 1.0)

    def swap(x):
        return pltpu.roll(x, HALF, axis=1)

    def times_i(x):
        return swap(x) * sign

    def minus_i(x):
        return swap(x) * (-sign)

    barrier = pltpu.get_barrier_semaphore()
    for step in range(1, devices):
        pl.semaphore_signal(
            barrier, inc=1, device_id=place(lax.rem(me + step, devices)), device_id_type=MESH
        )
    load_bins = pltpu.make_async_copy(bins, bins_raw, bins_load)
    load_bins.start()

    depth = staged.shape[1]
    chunks = slab // depth

    def stage(c):
        slot = lax.rem(c, 2)
        return pltpu.make_async_copy(
            density.at[pl.ds(c * depth, depth)], staged.at[slot], stage_sem.at[slot]
        )

    stage(0).start()
    scale = weight[0]

    def stage_step(c, carry):
        @pl.when(c + 1 < chunks)
        def _():
            stage(c + 1).start()

        stage(c).wait()
        slot = lax.rem(c, 2)

        def tile(i, carry):
            take = pl.ds(pl.multiple_of(i * TILE, TILE), TILE)
            xs = [staged[slot, take, b * LANES:(b + 1) * LANES] * scale for b in range(fold)]
            spec = real_fft(xs)
            put = pl.ds(pl.multiple_of(c * depth + i * TILE, TILE), TILE)
            folded[0, put, :LANES] = spec[0][0]
            folded[0, put, LANES:] = spec[slots][0]
            for k in range(1, slots):
                folded[k, put, :LANES] = spec[k][0]
                folded[k, put, LANES:] = spec[k][1]
            return carry

        return lax.fori_loop(0, depth // TILE, tile, carry, unroll=2)

    lax.fori_loop(0, chunks, stage_step, 0)

    side_plane = p // 2
    end, centre = (planes - 1) * side_plane, 1 + side_plane
    inner = planes - 1 - p
    is_end = lax.rem(p, planes - 1) == 0
    is_middle = lax.rem(p, planes - 1) > 0

    def sum_copy(which, dest):
        owner, target, to = (
            (planes - 1 - centre, outer_inner, centre),
            (centre, outer_own, centre),
            (planes - 1 - p, outer_far, centre),
            (inner, last_own, inner),
            (planes - 1 - end, inner_outer, inner),
            (end, last_own, end),
        )[which]
        return remote(
            parts.at[dest, owner], target.at[dest],
            sum_send.at[which, dest], sum_recv.at[which, dest], r * planes + to,
        )

    def sum_wait(which, dest):
        target = (outer_inner, outer_own, outer_far, last_own, inner_outer, last_own)[which]
        remote(
            target.at[dest], target.at[dest], sum_send.at[which, dest],
            sum_recv.at[which, dest], r * planes + lax.rem(p + 1, planes),
        ).wait_recv()

    def cross(dest):
        return remote(
            parts.at[dest, p], lines.at[pl.ds(r * blocks, blocks)],
            cross_send.at[dest], cross_recv.at[r], dest * planes + p,
        )

    def crossed(source):
        return remote(
            parts.at[source, p], lines.at[pl.ds(source * blocks, blocks)],
            cross_send.at[source], cross_recv.at[source], source * planes + p,
        )

    at_a = lax.broadcasted_iota(jnp.int32, (LANES, LANES), 0)

    def row_step(i, carry):
        dest = lax.rem(r + 1 + i, rows)
        for pair in range(pairs):
            k = dest * pairs + pair
            angle = (at_a * k).astype(F32) * angle_unit
            c, s = jnp.cos(angle), jnp.sin(angle)
            c, s = jnp.concatenate([c, c], 1), jnp.concatenate([s, s], 1)
            top, low = row_base[:LANES], row_base[LANES:]
            table[:LANES] = c * top - s * low
            table[LANES:] = c * low + s * top

            @pl.when(k == 0)
            def _():
                table[...] = row_zero[...]

            right = table[...]
            for q in range(blocks):
                done = dot3(folded[k, q * LANES:(q + 1) * LANES], right)
                parts[dest, 2 * pair, q] = done[:, :LANES]
                parts[dest, 2 * pair + 1, q] = done[:, LANES:]


        @pl.when(is_end)
        def _():
            sum_copy(2, dest).start()

        return carry

    pl.semaphore_wait(barrier, devices - 1)
    lax.fori_loop(0, rows, row_step, 0)

    def turn_of(i):
        return lax.rem(r + 1 + i, rows)

    @pl.when(is_end)
    def _():
        def near_step(i, carry):
            sum_copy(0, turn_of(i)).start()
            sum_copy(1, turn_of(i)).start()
            return carry

        lax.fori_loop(0, rows, near_step, 0)

    at_row = lax.broadcasted_iota(jnp.int32, (2 * LANES, 2 * LANES), 0)
    at_column = lax.broadcasted_iota(jnp.int32, (2 * LANES, 2 * LANES), 1)
    which_row = lax.rem(at_row // 4, 2)
    target = which_row * LANES + lax.rem(at_row, 4) * fold + at_row // 8
    table[...] = jnp.where(target == at_column, 1.0, 0.0)
    load_bins.wait()

    def bins_layout(k, carry):
        both = [bins_raw[pl.ds(2 * k + q, LANES, stride=fold), :] for q in range(2)]
        both = jnp.concatenate(both, 1).astype(F32).astype(BF16)
        out = lax.dot_general(
            table[...].astype(BF16), both, (((1,), (1,)), ((), ())), preferred_element_type=F32
        )
        bins_out[:, k] = out.reshape(fold, TILE, LANES)
        return carry

    lax.fori_loop(0, fold // 2, bins_layout, 0, unroll=2)
    side = me // slots

    def class_at(owner):
        k, h = owner // 2, lax.rem(owner, 2)
        other = k + lax.rem(h + side, 2) * (fold - 2 * k)
        return jnp.where(k == 0, h * slots, other)

    def send_bins(step):
        owner = lax.rem(me + step, devices)
        return remote(
            bins_out.at[class_at(owner)], bins_in.at[me],
            bins_send.at[step], bins_recv.at[step], owner,
        )

    def recv_bins(step):
        source = lax.rem(me + devices - step, devices)
        return remote(
            bins_out.at[0], bins_in.at[source], bins_send.at[step], bins_recv.at[step], source
        )

    def own_sum(dest):
        @pl.when(dest != r)
        def _():
            cross(dest).start()

    @pl.when(is_middle)
    def _():
        def far_relay(i, carry):
            @pl.when(i < rows)
            def _():
                dest = turn_of(i)
                sum_wait(2, dest)
                owner = planes - 1 - end
                parts[dest, owner] = parts[dest, owner] + outer_far[dest]
                sum_copy(4, dest).start()

            @pl.when(i > 0)
            def _():
                dest = turn_of(i - 1)
                sum_wait(4, dest)
                parts[dest, end] = parts[dest, end] + inner_outer[dest]
                sum_copy(5, dest).start()

            return carry

        lax.fori_loop(0, rows + 1, far_relay, 0)

    def bins_step(step, carry):
        send_bins(step).start()
        return carry

    lax.fori_loop(1, devices, bins_step, 0)
    bins_in[me] = bins_out[class_at(me)]

    @pl.when(is_middle)
    def _():
        def near_relay(i, carry):
            @pl.when(i < rows)
            def _():
                dest = turn_of(i)
                sum_wait(0, dest)
                parts[dest, inner] = parts[dest, inner] + outer_inner[dest]
                sum_copy(3, dest).start()

            @pl.when(i > 1)
            def _():
                dest = turn_of(i - 2)
                sum_wait(1, dest)
                sum_wait(3, dest)
                parts[dest, p] = parts[dest, p] + outer_own[dest] + last_own[dest]
                own_sum(dest)

            return carry

        lax.fori_loop(0, rows + 2, near_relay, 0)

    @pl.when(is_end)
    def _():
        def end_step(i, carry):
            dest = turn_of(i)
            sum_wait(5, dest)
            parts[dest, p] = parts[dest, p] + last_own[dest]
            own_sum(dest)
            return carry

        lax.fori_loop(0, rows, end_step, 0)

    def own_step(q, carry):
        lines[r * blocks + q] = parts[r, p, q]
        return carry

    lax.fori_loop(0, blocks, own_step, 0)

    def crossed_step(i, carry):
        crossed(lax.rem(r + rows - 1 - i, rows)).wait_recv()
        return carry

    lax.fori_loop(0, rows - 1, crossed_step, 0)

    def column_tile(i, carry):
        take = pl.ds(pl.multiple_of(i * TILE, TILE), TILE)
        spec = packed_fft([lines[b, take] for b in range(fold)], -1, swap, sign)
        lines[0, take] = spec[0]
        c1, s1 = turns[0, take], turns[1, take] * sign
        c, s = c1, s1
        for k in range(1, fold):
            lines[k, take] = spec[k] * c - swap(spec[k]) * s
            c, s = c * c1 - s * s1, s * c1 + c * s1
        return carry

    lax.fori_loop(0, LANES // TILE, column_tile, 0, unroll=2)

    k_me, h_me = me // 2, lax.rem(me, 2)
    index = lax.rem(lane, HALF)
    kx = jnp.where(
        k_me == 0, fold * index + h_me * slots, fold * (HALF * h_me + index) + k_me
    )
    across = jnp.where(kx >= length // 2, kx - length, kx).astype(F32)
    my = lax.broadcasted_iota(jnp.int32, (LANES, LANES), 0)
    at_lane = lax.broadcasted_iota(jnp.int32, (LANES, LANES), 1)
    pixel_scale = NBINS / float(length) ** 4

    def height_of(k):
        ky = k + fold * my
        return jnp.where(ky >= length // 2, ky - length, ky).astype(F32)

    def kernel_of(width, height):
        square_norm = height * height + width * width
        safe = jnp.where(square_norm == 0.0, 1.0, square_norm)
        inverse = 1.0 / safe
        return (width * width - height * height) * inverse, 2.0 * width * height * inverse

    def edge_of(k):
        return (my == HALF) & (k == 0)

    high, low = split(column[...])
    split_column[...] = jnp.concatenate([high, high, low], 1)

    def column_product(right):
        rh, rl = split(right)
        return jnp.dot(
            split_column[...], jnp.concatenate([rh, rl, rh], 0), preferred_element_type=F32
        )

    def each(f, x):
        count = x.shape[1] // LANES
        return jnp.concatenate([f(x[:, q * LANES:(q + 1) * LANES]) for q in range(count)], 1)

    def column_step(j, carry):
        z = jnp.concatenate([lines[2 * j], lines[2 * j + 1]], 1)
        both = column_product(jnp.concatenate([z, each(minus_i, z)], 0))
        turned = []
        for q in range(2):
            k = 2 * j + q
            v = both[:, q * LANES:(q + 1) * LANES]
            hat[k] = v
            square = v * v
            power[k] = (square + swap(square)) * pixel_scale
            kernel_real, kernel_imag = kernel_of(across, height_of(k))
            edge = edge_of(k)
            turned += [
                kernel_real * v + jnp.where(edge, kernel_imag * times_i(v), 0.0),
                jnp.where(edge, 0.0, kernel_imag * v),
            ]
        turned = jnp.concatenate(turned, 1)
        back = column_product(jnp.concatenate([turned, each(times_i, turned)], 0))
        shear[2 * j] = back[:, :2 * LANES]
        shear[2 * j + 1] = back[:, 2 * LANES:]
        return carry

    lax.fori_loop(0, fold // 2, column_step, 0, unroll=2)

    def reverse_of(wrap):
        return jnp.where(lax.rem(LANES - wrap - my, LANES) == at_lane, 1.0, 0.0).astype(BF16)

    @pl.when(me == 0)
    def _():
        spot = lax.rem(at_lane, HALF)

        def gather(k, held):
            return jnp.where(spot == k, pltpu.roll(hat[k], k, axis=1), held)

        v = lax.fori_loop(0, fold, gather, jnp.zeros((LANES, LANES), F32), unroll=2)
        high, low = split(v)

        def moved(wrap):
            mover = reverse_of(wrap)
            return jnp.dot(mover, high, preferred_element_type=F32) + jnp.dot(
                mover, low, preferred_element_type=F32
            )

        my_spot = lax.rem(my, HALF)
        same = (my // HALF == at_lane // HALF) & (spot < fold)
        partner = jnp.where(same & (lax.rem(fold - spot, fold) == my_spot), 1.0, 0.0)
        partner = partner.astype(BF16)
        high, low = split(jnp.where(spot == 0, moved(0), moved(1)))
        mirror = jnp.dot(high, partner, preferred_element_type=F32) + jnp.dot(
            low, partner, preferred_element_type=F32
        )
        mirror = mirror * (-sign)
        zero = jnp.where((my == 0) & (spot == 0), 0.0, (v + mirror) * 0.5)
        last = minus_i((v - mirror) * 0.5)
        zero_square, last_square = zero * zero, last * last
        powers = jnp.where(
            at_lane < HALF, zero_square + swap(zero_square), last_square + swap(last_square)
        ) * pixel_scale
        ky = spot + fold * my
        height = jnp.where(ky >= length // 2, ky - length, ky).astype(F32)
        kernel_real, kernel_imag = kernel_of(float(-(length // 2)), height)
        turned = times_i(kernel_real * last + kernel_imag * times_i(last))
        edge = ky == length // 2
        real = jnp.where(edge, 0.0, turned) - zero
        imag = jnp.where(edge, times_i(last), 0.0)
        both = jnp.concatenate([real, imag], 1)
        back = column_product(jnp.concatenate([both, each(times_i, both)], 0))

        def scatter(k, carry):
            shift = lax.rem(LANES - k, LANES)
            for part in range(2):
                span = slice(part * LANES, (part + 1) * LANES)
                value = pltpu.roll(back[:, span], shift, axis=1)
                shear[k, :, span] = jnp.where(spot == 0, value, shear[k, :, span])
            power[k] = jnp.where(spot == 0, pltpu.roll(powers, shift, axis=1), power[k])
            return carry

        lax.fori_loop(0, fold, scatter, 0, unroll=2)

    def inverse_tile(i, carry):
        take = pl.ds(pl.multiple_of(i * TILE, TILE), TILE)
        c1, s1 = turns[0, take], turns[1, take] * sign
        for part in range(2):
            span = slice(part * LANES, (part + 1) * LANES)
            c, s = c1, s1
            held = [shear[0, take, span]]
            for k in range(1, fold):
                value = shear[k, take, span]
                held.append(value * c + swap(value) * s)
                c, s = c * c1 - s * s1, s * c1 + c * s1
            for b, value in enumerate(packed_fft(held, 1, swap, sign)):
                shear[b, take, span] = value
        return carry

    lax.fori_loop(0, LANES // TILE, inverse_tile, 0, unroll=2)

    def give(dest):
        return remote(
            shear.at[dest], arrived.at[me], turn_send.at[dest], turn_recv.at[me], dest
        )

    def got(source):
        return remote(
            shear.at[source], arrived.at[source], turn_send.at[source], turn_recv.at[source],
            source,
        )

    for turn in (2, 1, 3, 0):
        def give_step(i, carry, turn=turn):
            give(lax.rem(r + i, rows) * planes + lax.rem(p + turn, planes)).start()
            return carry

        lax.fori_loop(1 if turn == 0 else 0, rows, give_step, 0)
    arrived[me] = shear[me]

    def bins_wait(step, carry):
        recv_bins(step).wait_recv()
        return carry

    lax.fori_loop(1, devices, bins_wait, 0)

    order = 4 * (at_row // 8) + lax.rem(at_row, 4)
    swapped = jnp.where(k_me == 0, 0, h_me)
    plain = lax.rem(1 - order // HALF + swapped, 2)
    origin = jnp.where((k_me == 0) & (h_me == 0), 2 * HALF, 2 * HALF - 1)
    inside = lax.rem(order, HALF)
    target = jnp.where(plain == 1, inside, HALF + lax.rem(origin - inside, HALF))
    target = target + which_row * LANES
    table[...] = jnp.where(target == at_column, 1.0, 0.0)

    def bins_turn(k, carry):
        block = bins_in[:, k].reshape(2 * LANES, LANES).astype(BF16)
        out = lax.dot_general(
            block, table[...].astype(BF16), (((0,), (0,)), ((), ())),
            preferred_element_type=F32,
        )
        bands[2 * k] = out[:, :LANES]
        bands[2 * k + 1] = out[:, LANES:]
        return carry

    lax.fori_loop(0, fold // 2, bins_turn, 0, unroll=2)
    sums[...] = jnp.zeros_like(sums)

    def band_step(k, carry):
        flipped = jnp.dot(
            reverse_of(jnp.where(k == 0, 0, 1)), bands[lax.rem(fold - k, fold)].astype(BF16),
            preferred_element_type=F32,
        )
        band = jnp.where(lane < HALF, bands[k], flipped)
        energy = power[k]
        for b in range(NBINS):
            kept = jnp.where(band == float(b), energy, 0.0)
            sums[b] += jnp.sum(kept.reshape(LANES // TILE, TILE, LANES), axis=0)
        return carry

    lax.fori_loop(0, fold, band_step, 0)
    totals = jnp.sum(jnp.sum(sums[...], axis=1), axis=1, keepdims=True)
    diagonal = lax.broadcasted_iota(jnp.int32, (NBINS, LANES), 0) == lax.broadcasted_iota(
        jnp.int32, (NBINS, LANES), 1
    )
    line = jnp.sum(jnp.where(diagonal, totals, 0.0), axis=0, keepdims=True)
    sums_out[...] = jnp.broadcast_to(line, (TILE, LANES))
    sums_in[me] = jnp.broadcast_to(line, (TILE, LANES))

    def tell(step):
        dest = lax.rem(me + step, devices)
        return remote(sums_out, sums_in.at[me], total_send.at[step], total_recv.at[step], dest)

    def told(step):
        source = lax.rem(me + devices - step, devices)
        return remote(
            sums_out, sums_in.at[source], total_send.at[step], total_recv.at[step], source
        )

    def tell_step(step, carry):
        tell(step).start()
        return carry

    lax.fori_loop(1, devices, tell_step, 0)

    def back_step(i, carry):
        k = lax.rem(me // 2 + slots - i, slots)
        for h in range(2):
            @pl.when(2 * k + h != me)
            def _():
                got(2 * k + h).wait_recv()

        angle = (lane * k).astype(F32) * angle_unit
        c, s = jnp.cos(angle), jnp.sin(angle)
        cos, sin = back_base[:, :LANES], back_base[:, LANES:]
        table[:, :LANES] = cos * c - sin * s
        table[:, LANES:] = sin * c + cos * s

        @pl.when(k == 0)
        def _():
            table[...] = back_zero[...]

        left = [
            jnp.concatenate(
                [arrived[2 * k + h, :, part * LANES:(part + 1) * LANES] for h in range(2)], 1
            )
            for part in range(2)
        ]
        folded[k, :2 * LANES] = dot3(jnp.concatenate(left, 0), table[...])
        return carry

    lax.fori_loop(0, slots, back_step, 0, unroll=2)

    for part, out in enumerate((out_real, out_imag)):
        def back_tile(i, carry, part=part, out=out):
            take = pl.ds(pl.multiple_of(part * LANES + i * TILE, TILE), TILE)
            spec = [(folded[0, take, :LANES], None)]
            for k in range(1, slots):
                spec.append((folded[k, take, :LANES], folded[k, take, LANES:]))
            spec.append((folded[0, take, LANES:], None))
            put = pl.ds(pl.multiple_of(i * TILE, TILE), TILE)
            for b, value in enumerate(real_inverse(spec, fold)):
                out[put, b * LANES:(b + 1) * LANES] = value
            return carry

        lax.fori_loop(0, LANES // TILE, back_tile, 0, unroll=2)

    def told_step(step, carry):
        told(step).wait_recv()
        return carry

    lax.fori_loop(1, devices, told_step, 0)
    out_spectrum[...] = jnp.sum(sums_in[...], axis=0)

    def last_step(step, carry):
        give(lax.rem(me + step, devices)).wait_send()
        tell(step).wait_send()
        send_bins(step).wait_send()
        return carry

    lax.fori_loop(1, devices, last_step, 0)

    def sent_step(dest, carry):
        @pl.when(is_end)
        def _():
            for which in (0, 1, 2):
                sum_copy(which, dest).wait_send()

        @pl.when(is_middle)
        def _():
            for which in (3, 4, 5):
                sum_copy(which, dest).wait_send()

        @pl.when(dest != r)
        def _():
            cross(dest).wait_send()

        return carry

    lax.fori_loop(0, rows, sent_step, 0)


def folded_device(density, lens_weight, spectrum_bin):
    rows, planes = lax.axis_size("rows"), lax.axis_size("planes")
    devices = rows * planes
    slab, length = density.shape[1:]
    fold, blocks, slots = devices, slab // LANES, devices // 2
    row_base, row_zero = row_tables(fold)
    back_base, back_zero = back_tables(fold)
    vmem = pl.BlockSpec(memory_space=pltpu.VMEM)
    hbm = pl.BlockSpec(memory_space=pl.ANY)
    smem = pl.BlockSpec(memory_space=pltpu.SMEM)
    dma = pltpu.SemaphoreType.DMA
    chunk = (blocks, LANES, LANES)
    scratch = [
        pltpu.VMEM((2, min(64, slab), length), F32),
        pltpu.VMEM((slots, slab, 2 * LANES), F32),
        pltpu.VMEM((rows, planes) + chunk, F32),
        pltpu.VMEM((rows,) + chunk, F32),
        pltpu.VMEM((rows,) + chunk, F32),
        pltpu.VMEM((rows,) + chunk, F32),
        pltpu.VMEM((rows,) + chunk, F32),
        pltpu.VMEM((rows,) + chunk, F32),
        pltpu.VMEM((fold, LANES, LANES), F32),
        pltpu.VMEM((fold, LANES, LANES), F32),
        pltpu.VMEM((fold, LANES, 2 * LANES), F32),
        pltpu.VMEM((fold, LANES, LANES), F32),
        pltpu.VMEM((devices, LANES, 2 * LANES), F32),
        pltpu.VMEM((length, LANES), jnp.int32),
        pltpu.VMEM((fold, fold // 2, TILE, LANES), F32),
        pltpu.VMEM((devices, fold // 2, TILE, LANES), F32),
        pltpu.VMEM((fold, LANES, LANES), F32),
        pltpu.VMEM((NBINS, TILE, LANES), F32),
        pltpu.VMEM((TILE, LANES), F32),
        pltpu.VMEM((devices, TILE, LANES), F32),
        pltpu.VMEM((2 * LANES, 2 * LANES), F32),
        pltpu.VMEM((LANES, 6 * LANES), BF16),
        dma((2,)),
        dma((6, rows)), dma((6, rows)),
        dma((rows,)), dma((rows,)),
        dma((devices,)), dma((devices,)), dma,
        dma((devices,)), dma((devices,)),
        dma((devices,)), dma((devices,)),
    ]
    real, imag, spectrum = pl.pallas_call(
        functools.partial(shear_kernel, rows, planes, slab),
        out_shape=(
            jax.ShapeDtypeStruct((length // devices, length), F32),
            jax.ShapeDtypeStruct((length // devices, length), F32),
            jax.ShapeDtypeStruct((TILE, LANES), F32),
        ),
        in_specs=[hbm, smem, hbm] + [vmem] * 6,
        out_specs=(vmem, vmem, vmem),
        scratch_shapes=scratch,
        compiler_params=pltpu.CompilerParams(
            collective_id=0, has_side_effects=True, vmem_limit_bytes=67043328
        ),
        name="shear",
    )(
        density[0], lens_weight, spectrum_bin,
        row_base, row_zero, back_base, back_zero, column_table(), turn_table(length),
    )
    return real, imag, spectrum[0, :NBINS]


def phase(left, right, length, orient):
    index = np.arange(left)[:, None] * np.arange(right)[None, :] % length
    return np.exp(orient * 2j * math.pi * index / length)


def as_blocks(table):
    rows = np.stack([table.real, -table.imag], -1), np.stack([table.imag, table.real], -1)
    return np.stack(rows, 1).astype(np.float32)


def lane_table(table):
    top = np.concatenate([table.real, table.imag], 1)
    bottom = np.concatenate([-table.imag, table.real], 1)
    return np.concatenate([top, bottom], 0).astype(np.float32)


def product(pattern, left, right):
    return jnp.einsum(pattern, left, right, precision=lax.Precision.HIGH)


def turn(real, imag, table):
    cos, sin = table.real.astype(np.float32), table.imag.astype(np.float32)
    return real * cos - imag * sin, real * sin + imag * cos


def centred(indices, length):
    return ((indices + length // 2) % length - length // 2).astype(jnp.float32)


def plane_sum(density, lens_weight):
    count = lax.axis_size("planes")
    here = lax.axis_index("planes")
    block = density.shape[1] // count
    half = block // 2

    def own(owner, part):
        start = (owner % count) * block + part * half
        piece = lax.dynamic_slice_in_dim(density, start, half, axis=1)
        return jnp.sum(piece * lens_weight[:, None, None], axis=0)

    ways = ((0, 1), (1, -1))
    held = [own(here - way + count, part) for part, way in ways]
    for step in range(count - 1):
        moved = [
            lax.ppermute(held[part], "planes", [(i, (i + way) % count) for i in range(count)])
            for part, way in ways
        ]
        held = [
            moved[part] + own(here - way * (2 + step) + 2 * count, part) for part, way in ways
        ]
    return jnp.concatenate(held, axis=0)


def on_device(density, lens_weight, spectrum_bin):
    length = density.shape[-1]
    devices = lax.axis_size("rows") * lax.axis_size("planes")
    narrow = length // devices
    me = lax.axis_index("rows") * lax.axis_size("planes") + lax.axis_index("planes")

    share = plane_sum(density, lens_weight)
    field = share.T.reshape(narrow, devices, narrow)
    first = phase(narrow, narrow, narrow, -1)
    real = product("kn,nqy->kqy", first.real.astype(np.float32), field)
    imag = product("kn,nqy->kqy", first.imag.astype(np.float32), field)
    real, imag = turn(real, imag, phase(narrow, devices, length, -1)[:, :, None])
    forward = as_blocks(phase(devices, devices, devices, -1))
    spread = product("leq,kqy->leky", forward[..., 0], real) + product(
        "leq,kqy->leky", forward[..., 1], imag
    )
    held = lax.all_to_all(spread, AXES, split_axis=0, concat_axis=0, tiled=True)

    held = product("kesc,scxt->kext", forward, held)
    real, imag = turn(held[:, 0], held[:, 1], phase(devices, narrow, length, -1)[:, None, :])
    hat = product(
        "kxt,tm->kxm",
        jnp.concatenate([real, imag], -1),
        lane_table(phase(narrow, narrow, narrow, -1)),
    )
    hat_real, hat_imag = hat[..., :narrow], hat[..., narrow:]

    ky_index = (
        jnp.arange(devices, dtype=jnp.int32)[:, None, None]
        + devices * jnp.arange(narrow, dtype=jnp.int32)[None, None, :]
    )
    height = centred(ky_index, length)
    across = centred(me * narrow + jnp.arange(narrow, dtype=jnp.int32), length)[None, :, None]
    square_norm = height**2 + across**2
    anchor = square_norm == 0
    safe_norm = jnp.where(anchor, 1.0, square_norm)
    hat_real = jnp.where(anchor, 0.0, hat_real)
    hat_imag = jnp.where(anchor, 0.0, hat_imag)

    kernel_real = (across**2 - height**2) / safe_norm
    kernel_imag = 2.0 * across * height / safe_norm
    shear = jnp.concatenate(
        [
            kernel_real * hat_real - kernel_imag * hat_imag,
            kernel_real * hat_imag + kernel_imag * hat_real,
        ],
        -1,
    )
    back = product(
        "kxm,mt->kxt", shear, lane_table(phase(narrow, narrow, narrow, 1) / length)
    )
    real, imag = turn(
        back[..., :narrow], back[..., narrow:], phase(devices, narrow, length, 1)[:, None, :]
    )
    inverse = as_blocks(phase(devices, devices, devices, 1))
    back = product("sek,kxt->sext", inverse[..., 0], real) + product(
        "sek,kxt->sext", inverse[..., 1], imag
    )
    turned = lax.all_to_all(back, AXES, split_axis=0, concat_axis=0, tiled=True)

    pixel_power = (hat_real**2 + hat_imag**2) * (NBINS / float(length) ** 4)
    bins = spectrum_bin.reshape(narrow, devices, narrow).transpose(1, 2, 0)
    band_ids = jnp.arange(NBINS, dtype=jnp.int32)[:, None, None, None]
    partial_power = jnp.sum(jnp.where(bins == band_ids, pixel_power, 0.0), axis=(1, 2, 3))
    copies = jnp.broadcast_to(partial_power, (devices, 8, NBINS))
    gathered = lax.all_to_all(copies, AXES, split_axis=0, concat_axis=0, tiled=True)
    spectrum = jnp.sum(gathered[:, 0, :], axis=0)

    turned = product("aedc,dcqt->aeqt", inverse, turned)
    real, imag = turn(
        turned[:, 0], turned[:, 1], phase(devices, narrow, length, 1)[:, :, None]
    )
    last = phase(narrow, narrow, narrow, 1) / length
    cos, sin = last.real.astype(np.float32), last.imag.astype(np.float32)
    out_real = product("bq,aqt->bat", cos, real) - product("bq,aqt->bat", sin, imag)
    out_imag = product("bq,aqt->bat", sin, real) + product("bq,aqt->bat", cos, imag)
    shape = (length, narrow)
    return (out_real.reshape(shape).T, out_imag.reshape(shape).T, spectrum)


def folds(mesh, density):
    rows, planes = mesh.shape["rows"], mesh.shape["planes"]
    count, length, width = density.shape
    return (
        count == planes
        and planes == 4
        and length == width == LANES * rows * planes
        and rows * planes == LANES // 4
    )


def solution(mesh):
    specs = (P("planes", "rows", None), P("planes"), P(None, AXES))
    outs = (P(AXES, None), P(AXES, None), P())

    def run(density, lens_weight, spectrum_bin):
        if folds(mesh, density):
            body = folded_device
        else:
            body = on_device
        whole = jax.shard_map(body, mesh=mesh, in_specs=specs, out_specs=outs, check_vma=False)
        return whole(density, lens_weight, spectrum_bin)

    return run
```

```python
import functools
import math

import jax
import jax.numpy as jnp
import numpy as np
from jax import lax
from jax.experimental import pallas as pl
from jax.experimental.pallas import tpu as pltpu
from jax.sharding import PartitionSpec as P

NBINS = 64
AXES = ("rows", "planes")
LANES = 128
HALF = LANES // 2
TILE = 8
MESH = pl.DeviceIdType.MESH
F32 = jnp.float32
BF16 = jnp.bfloat16


def real_fft(xs):
    n = len(xs)
    if n == 2:
        return [(xs[0] + xs[1], None), (xs[0] - xs[1], None)]
    even, odd = real_fft(xs[0::2]), real_fft(xs[1::2])
    out = [None] * (n // 2 + 1)
    out[0] = (even[0][0] + odd[0][0], None)
    out[n // 2] = (even[0][0] - odd[0][0], None)
    out[n // 4] = (even[n // 4][0], -odd[n // 4][0])
    for k in range(1, n // 4):
        c, s = math.cos(2 * math.pi * k / n), math.sin(2 * math.pi * k / n)
        (er, ei), (odr, odi) = even[k], odd[k]
        tr, ti = c * odr + s * odi, c * odi - s * odr
        out[k] = (er + tr, ei + ti)
        out[n // 2 - k] = (er - tr, ti - ei)
    return out


def real_inverse(spec, n):
    if n == 2:
        return [spec[0][0] + spec[1][0], spec[0][0] - spec[1][0]]
    h, q = n // 2, n // 4
    even, odd = [None] * (q + 1), [None] * (q + 1)
    even[0] = (spec[0][0] + spec[h][0], None)
    odd[0] = (spec[0][0] - spec[h][0], None)
    even[q] = (2.0 * spec[q][0], None)
    odd[q] = (-2.0 * spec[q][1], None)
    for k in range(1, q):
        (ar, ai), (br, bi) = spec[k], spec[h - k]
        even[k] = (ar + br, ai - bi)
        ur, ui = ar - br, ai + bi
        c, s = math.cos(2 * math.pi * k / n), math.sin(2 * math.pi * k / n)
        odd[k] = (c * ur - s * ui, c * ui + s * ur)
    evens, odds = real_inverse(even, h), real_inverse(odd, h)
    out = [None] * n
    out[0::2], out[1::2] = evens, odds
    return out


def packed_fft(xs, orient, swap, sign):
    n = len(xs)
    if n == 1:
        return xs
    even = packed_fft(xs[0::2], orient, swap, sign)
    odd = packed_fft(xs[1::2], orient, swap, sign)
    out = [None] * n
    for k in range(n // 2):
        c, s = math.cos(2 * math.pi * k / n), orient * math.sin(2 * math.pi * k / n)
        if k == 0:
            t = odd[0]
        elif 4 * k == n:
            t = swap(odd[k]) * (orient * sign)
        else:
            t = c * odd[k] + swap(odd[k]) * (s * sign)
        out[k], out[k + n // 2] = even[k] + t, even[k] - t
    return out


def split(x):
    high = x.astype(BF16)
    return high, (x - high.astype(F32)).astype(BF16)


def dot3(left, right):
    lh, ll = split(left)
    rh, rl = split(right)
    return jnp.dot(
        jnp.concatenate([lh, lh, ll], 1),
        jnp.concatenate([rh, rl, rh], 0),
        preferred_element_type=F32,
    )


def row_tables(fold):
    length = fold * LANES
    a = np.arange(LANES)
    general = np.zeros((2, LANES, 2, 2, HALF))
    special = np.zeros((2, LANES, 2, 2, HALF))
    for h in range(2):
        m = h * HALF + np.arange(HALF)
        angle = 2 * np.pi * (a[:, None] * m[None, :] % LANES) / LANES
        general[0, :, h, 0], general[0, :, h, 1] = np.cos(angle), -np.sin(angle)
        general[1, :, h, 0], general[1, :, h, 1] = np.sin(angle), np.cos(angle)
        kx = fold * np.arange(HALF) + h * (fold // 2)
        angle = 2 * np.pi * (a[:, None] * kx[None, :] % length) / length
        special[h, :, h, 0], special[h, :, h, 1] = np.cos(angle), -np.sin(angle)
    special[0, :, 0, 1, 0] = 1 - 2 * (a % 2)
    shape = (2 * LANES, 2 * LANES)
    return general.reshape(shape).astype(np.float32), special.reshape(shape).astype(np.float32)


def back_tables(fold):
    length = fold * LANES
    a = np.arange(LANES)
    general = np.zeros((2, 2, HALF, 2, LANES))
    special = np.zeros((2, 2, HALF, 2, LANES))
    for h in range(2):
        m = h * HALF + np.arange(HALF)
        angle = 2 * np.pi * (m[:, None] * a[None, :] % LANES) / LANES
        general[h, 0, :, 0], general[h, 0, :, 1] = np.cos(angle), np.sin(angle)
        general[h, 1, :, 0], general[h, 1, :, 1] = -np.sin(angle), np.cos(angle)
        kx = fold * np.arange(HALF) + h * (fold // 2)
        angle = 2 * np.pi * (kx[:, None] * a[None, :] % length) / length
        special[h, 0, :, h], special[h, 1, :, h] = 2 * np.cos(angle), -2 * np.sin(angle)
    special[0, 0, 0, 0] = 1.0
    special[0, 1, 0, 0] = 1 - 2 * (a % 2)
    shape, scale = (2 * LANES, 2 * LANES), float(length) ** -2
    return (
        (general.reshape(shape) * scale).astype(np.float32),
        (special.reshape(shape) * scale).astype(np.float32),
    )


def column_table():
    a = np.arange(LANES)
    angle = 2 * np.pi * (a[:, None] * a[None, :] % LANES) / LANES
    return np.concatenate([np.cos(angle), np.sin(angle)], 1).astype(np.float32)


def turn_table(length):
    angle = 2 * np.pi * np.arange(LANES)[:, None] / length * np.ones((1, LANES))
    return np.stack([np.cos(angle), np.sin(angle)]).astype(np.float32)


def shear_kernel(
    rows, planes, slab,
    density, weight, bins, row_base, row_zero, back_base, back_zero, column, turns,
    out_real, out_imag, out_spectrum,
    staged, folded, parts, outer_inner, outer_own, outer_far, inner_outer, last_own, lines, hat, shear, power,
    arrived, bins_raw, bins_out, bins_in, bands, sums, sums_out, sums_in, table, split_column,
    stage_sem, sum_send, sum_recv, cross_send, cross_recv,
    bins_send, bins_recv, bins_load, turn_send, turn_recv, total_send, total_recv,
):
    devices = rows * planes
    fold = devices
    length = fold * LANES
    slots = fold // 2
    blocks = slab // LANES
    pairs = planes // 2
    angle_unit = 2 * math.pi / length
    r, p = lax.axis_index("rows"), lax.axis_index("planes")
    me = r * planes + p

    def place(device):
        return {"rows": device // planes, "planes": lax.rem(device, planes)}

    def remote(source, target, send, recv, device):
        return pltpu.make_async_remote_copy(
            source, target, send, recv, device_id=place(device), device_id_type=MESH
        )

    lane = lax.broadcasted_iota(jnp.int32, (1, LANES), 1)
    sign = jnp.where(lane < HALF, -1.0, 1.0)

    def swap(x):
        return pltpu.roll(x, HALF, axis=1)

    def times_i(x):
        return swap(x) * sign

    def minus_i(x):
        return swap(x) * (-sign)

    barrier = pltpu.get_barrier_semaphore()
    for step in range(1, devices):
        pl.semaphore_signal(
            barrier, inc=1, device_id=place(lax.rem(me + step, devices)), device_id_type=MESH
        )
    load_bins = pltpu.make_async_copy(bins, bins_raw, bins_load)
    load_bins.start()

    depth = staged.shape[1]
    chunks = slab // depth

    def stage(c):
        slot = lax.rem(c, 2)
        return pltpu.make_async_copy(
            density.at[pl.ds(c * depth, depth)], staged.at[slot], stage_sem.at[slot]
        )

    stage(0).start()
    scale = weight[0]

    def stage_step(c, carry):
        @pl.when(c + 1 < chunks)
        def _():
            stage(c + 1).start()

        stage(c).wait()
        slot = lax.rem(c, 2)

        def tile(i, carry):
            take = pl.ds(pl.multiple_of(i * TILE, TILE), TILE)
            xs = [staged[slot, take, b * LANES:(b + 1) * LANES] * scale for b in range(fold)]
            spec = real_fft(xs)
            put = pl.ds(pl.multiple_of(c * depth + i * TILE, TILE), TILE)
            folded[0, put, :LANES] = spec[0][0]
            folded[0, put, LANES:] = spec[slots][0]
            for k in range(1, slots):
                folded[k, put, :LANES] = spec[k][0]
                folded[k, put, LANES:] = spec[k][1]
            return carry

        return lax.fori_loop(0, depth // TILE, tile, carry, unroll=2)

    lax.fori_loop(0, chunks, stage_step, 0)

    side_plane = p // 2
    end, centre = (planes - 1) * side_plane, 1 + side_plane
    inner = planes - 1 - p
    is_end = lax.rem(p, planes - 1) == 0
    is_middle = lax.rem(p, planes - 1) > 0

    def sum_copy(which, dest):
        owner, target, to = (
            (planes - 1 - centre, outer_inner, centre),
            (centre, outer_own, centre),
            (planes - 1 - p, outer_far, centre),
            (inner, last_own, inner),
            (planes - 1 - end, inner_outer, inner),
            (end, last_own, end),
        )[which]
        return remote(
            parts.at[dest, owner], target.at[dest],
            sum_send.at[which, dest], sum_recv.at[which, dest], r * planes + to,
        )

    def sum_wait(which, dest):
        target = (outer_inner, outer_own, outer_far, last_own, inner_outer, last_own)[which]
        remote(
            target.at[dest], target.at[dest], sum_send.at[which, dest],
            sum_recv.at[which, dest], r * planes + lax.rem(p + 1, planes),
        ).wait_recv()

    def cross(dest):
        return remote(
            parts.at[dest, p], lines.at[pl.ds(r * blocks, blocks)],
            cross_send.at[dest], cross_recv.at[r], dest * planes + p,
        )

    def crossed(source):
        return remote(
            parts.at[source, p], lines.at[pl.ds(source * blocks, blocks)],
            cross_send.at[source], cross_recv.at[source], source * planes + p,
        )

    at_a = lax.broadcasted_iota(jnp.int32, (LANES, LANES), 0)

    def row_step(i, carry):
        dest = lax.rem(r + 1 + i, rows)
        for pair in range(pairs):
            k = dest * pairs + pair
            angle = (at_a * k).astype(F32) * angle_unit
            c, s = jnp.cos(angle), jnp.sin(angle)
            c, s = jnp.concatenate([c, c], 1), jnp.concatenate([s, s], 1)
            top, low = row_base[:LANES], row_base[LANES:]
            table[:LANES] = c * top - s * low
            table[LANES:] = c * low + s * top

            @pl.when(k == 0)
            def _():
                table[...] = row_zero[...]

            right = table[...]
            for q in range(blocks):
                done = dot3(folded[k, q * LANES:(q + 1) * LANES], right)
                parts[dest, 2 * pair, q] = done[:, :LANES]
                parts[dest, 2 * pair + 1, q] = done[:, LANES:]


        @pl.when(is_end)
        def _():
            sum_copy(2, dest).start()

        return carry

    pl.semaphore_wait(barrier, devices - 1)
    lax.fori_loop(0, rows, row_step, 0)

    def turn_of(i):
        return lax.rem(r + 1 + i, rows)

    @pl.when(is_end)
    def _():
        def near_step(i, carry):
            sum_copy(0, turn_of(i)).start()
            sum_copy(1, turn_of(i)).start()
            return carry

        lax.fori_loop(0, rows, near_step, 0)

    at_row = lax.broadcasted_iota(jnp.int32, (2 * LANES, 2 * LANES), 0)
    at_column = lax.broadcasted_iota(jnp.int32, (2 * LANES, 2 * LANES), 1)
    which_row = lax.rem(at_row // 4, 2)
    target = which_row * LANES + lax.rem(at_row, 4) * fold + at_row // 8
    table[...] = jnp.where(target == at_column, 1.0, 0.0)
    load_bins.wait()

    def bins_layout(k, carry):
        both = [bins_raw[pl.ds(2 * k + q, LANES, stride=fold), :] for q in range(2)]
        both = jnp.concatenate(both, 1).astype(F32).astype(BF16)
        out = lax.dot_general(
            table[...].astype(BF16), both, (((1,), (1,)), ((), ())), preferred_element_type=F32
        )
        bins_out[:, k] = out.reshape(fold, TILE, LANES)
        return carry

    lax.fori_loop(0, fold // 2, bins_layout, 0, unroll=2)
    side = me // slots

    def class_at(owner):
        k, h = owner // 2, lax.rem(owner, 2)
        other = k + lax.rem(h + side, 2) * (fold - 2 * k)
        return jnp.where(k == 0, h * slots, other)

    def send_bins(step):
        owner = lax.rem(me + step, devices)
        return remote(
            bins_out.at[class_at(owner)], bins_in.at[me],
            bins_send.at[step], bins_recv.at[step], owner,
        )

    def recv_bins(step):
        source = lax.rem(me + devices - step, devices)
        return remote(
            bins_out.at[0], bins_in.at[source], bins_send.at[step], bins_recv.at[step], source
        )

    def own_sum(dest):
        @pl.when(dest != r)
        def _():
            cross(dest).start()

    @pl.when(is_middle)
    def _():
        def far_relay(i, carry):
            @pl.when(i < rows)
            def _():
                dest = turn_of(i)
                sum_wait(2, dest)
                owner = planes - 1 - end
                parts[dest, owner] = parts[dest, owner] + outer_far[dest]
                sum_copy(4, dest).start()

            @pl.when(i > 0)
            def _():
                dest = turn_of(i - 1)
                sum_wait(4, dest)
                parts[dest, end] = parts[dest, end] + inner_outer[dest]
                sum_copy(5, dest).start()

            return carry

        lax.fori_loop(0, rows + 1, far_relay, 0)

    def bins_step(step, carry):
        send_bins(step).start()
        return carry

    @pl.when(is_middle)
    def _():
        lax.fori_loop(1, devices, bins_step, 0)

    bins_in[me] = bins_out[class_at(me)]

    @pl.when(is_middle)
    def _():
        def near_relay(i, carry):
            @pl.when(i < rows)
            def _():
                dest = turn_of(i)
                sum_wait(0, dest)
                parts[dest, inner] = parts[dest, inner] + outer_inner[dest]
                sum_copy(3, dest).start()

            @pl.when(i > 1)
            def _():
                dest = turn_of(i - 2)
                sum_wait(1, dest)
                sum_wait(3, dest)
                parts[dest, p] = parts[dest, p] + outer_own[dest] + last_own[dest]
                own_sum(dest)

            return carry

        lax.fori_loop(0, rows + 2, near_relay, 0)

    @pl.when(is_end)
    def _():
        def end_step(i, carry):
            dest = turn_of(i)
            sum_wait(5, dest)
            parts[dest, p] = parts[dest, p] + last_own[dest]
            own_sum(dest)
            return carry

        lax.fori_loop(0, rows, end_step, 0)

    def own_step(q, carry):
        lines[r * blocks + q] = parts[r, p, q]
        return carry

    lax.fori_loop(0, blocks, own_step, 0)

    def crossed_step(i, carry):
        crossed(lax.rem(r + rows - 1 - i, rows)).wait_recv()
        return carry

    lax.fori_loop(0, rows - 1, crossed_step, 0)

    def column_tile(i, carry):
        take = pl.ds(pl.multiple_of(i * TILE, TILE), TILE)
        spec = packed_fft([lines[b, take] for b in range(fold)], -1, swap, sign)
        lines[0, take] = spec[0]
        c1, s1 = turns[0, take], turns[1, take] * sign
        c, s = c1, s1
        for k in range(1, fold):
            lines[k, take] = spec[k] * c - swap(spec[k]) * s
            c, s = c * c1 - s * s1, s * c1 + c * s1
        return carry

    lax.fori_loop(0, LANES // TILE, column_tile, 0, unroll=2)

    k_me, h_me = me // 2, lax.rem(me, 2)
    index = lax.rem(lane, HALF)
    kx = jnp.where(
        k_me == 0, fold * index + h_me * slots, fold * (HALF * h_me + index) + k_me
    )
    across = jnp.where(kx >= length // 2, kx - length, kx).astype(F32)
    my = lax.broadcasted_iota(jnp.int32, (LANES, LANES), 0)
    at_lane = lax.broadcasted_iota(jnp.int32, (LANES, LANES), 1)
    pixel_scale = NBINS / float(length) ** 4

    def height_of(k):
        ky = k + fold * my
        return jnp.where(ky >= length // 2, ky - length, ky).astype(F32)

    def kernel_of(width, height):
        square_norm = height * height + width * width
        safe = jnp.where(square_norm == 0.0, 1.0, square_norm)
        inverse = 1.0 / safe
        return (width * width - height * height) * inverse, 2.0 * width * height * inverse

    def edge_of(k):
        return (my == HALF) & (k == 0)

    high, low = split(column[...])
    split_column[...] = jnp.concatenate([high, high, low], 1)

    def column_product(right):
        rh, rl = split(right)
        return jnp.dot(
            split_column[...], jnp.concatenate([rh, rl, rh], 0), preferred_element_type=F32
        )

    def each(f, x):
        count = x.shape[1] // LANES
        return jnp.concatenate([f(x[:, q * LANES:(q + 1) * LANES]) for q in range(count)], 1)

    def column_step(j, carry):
        z = jnp.concatenate([lines[2 * j], lines[2 * j + 1]], 1)
        both = column_product(jnp.concatenate([z, each(minus_i, z)], 0))
        turned = []
        for q in range(2):
            k = 2 * j + q
            v = both[:, q * LANES:(q + 1) * LANES]
            hat[k] = v
            square = v * v
            power[k] = (square + swap(square)) * pixel_scale
            kernel_real, kernel_imag = kernel_of(across, height_of(k))
            edge = edge_of(k)
            turned += [
                kernel_real * v + jnp.where(edge, kernel_imag * times_i(v), 0.0),
                jnp.where(edge, 0.0, kernel_imag * v),
            ]
        turned = jnp.concatenate(turned, 1)
        back = column_product(jnp.concatenate([turned, each(times_i, turned)], 0))
        shear[2 * j] = back[:, :2 * LANES]
        shear[2 * j + 1] = back[:, 2 * LANES:]
        return carry

    lax.fori_loop(0, fold // 2, column_step, 0, unroll=2)

    def reverse_of(wrap):
        return jnp.where(lax.rem(LANES - wrap - my, LANES) == at_lane, 1.0, 0.0).astype(BF16)

    @pl.when(me == 0)
    def _():
        spot = lax.rem(at_lane, HALF)

        def gather(k, held):
            return jnp.where(spot == k, pltpu.roll(hat[k], k, axis=1), held)

        v = lax.fori_loop(0, fold, gather, jnp.zeros((LANES, LANES), F32), unroll=2)
        high, low = split(v)

        def moved(wrap):
            mover = reverse_of(wrap)
            return jnp.dot(mover, high, preferred_element_type=F32) + jnp.dot(
                mover, low, preferred_element_type=F32
            )

        my_spot = lax.rem(my, HALF)
        same = (my // HALF == at_lane // HALF) & (spot < fold)
        partner = jnp.where(same & (lax.rem(fold - spot, fold) == my_spot), 1.0, 0.0)
        partner = partner.astype(BF16)
        high, low = split(jnp.where(spot == 0, moved(0), moved(1)))
        mirror = jnp.dot(high, partner, preferred_element_type=F32) + jnp.dot(
            low, partner, preferred_element_type=F32
        )
        mirror = mirror * (-sign)
        zero = jnp.where((my == 0) & (spot == 0), 0.0, (v + mirror) * 0.5)
        last = minus_i((v - mirror) * 0.5)
        zero_square, last_square = zero * zero, last * last
        powers = jnp.where(
            at_lane < HALF, zero_square + swap(zero_square), last_square + swap(last_square)
        ) * pixel_scale
        ky = spot + fold * my
        height = jnp.where(ky >= length // 2, ky - length, ky).astype(F32)
        kernel_real, kernel_imag = kernel_of(float(-(length // 2)), height)
        turned = times_i(kernel_real * last + kernel_imag * times_i(last))
        edge = ky == length // 2
        real = jnp.where(edge, 0.0, turned) - zero
        imag = jnp.where(edge, times_i(last), 0.0)
        both = jnp.concatenate([real, imag], 1)
        back = column_product(jnp.concatenate([both, each(times_i, both)], 0))

        def scatter(k, carry):
            shift = lax.rem(LANES - k, LANES)
            for part in range(2):
                span = slice(part * LANES, (part + 1) * LANES)
                value = pltpu.roll(back[:, span], shift, axis=1)
                shear[k, :, span] = jnp.where(spot == 0, value, shear[k, :, span])
            power[k] = jnp.where(spot == 0, pltpu.roll(powers, shift, axis=1), power[k])
            return carry

        lax.fori_loop(0, fold, scatter, 0, unroll=2)

    def inverse_tile(i, carry):
        take = pl.ds(pl.multiple_of(i * TILE, TILE), TILE)
        c1, s1 = turns[0, take], turns[1, take] * sign
        for part in range(2):
            span = slice(part * LANES, (part + 1) * LANES)
            c, s = c1, s1
            held = [shear[0, take, span]]
            for k in range(1, fold):
                value = shear[k, take, span]
                held.append(value * c + swap(value) * s)
                c, s = c * c1 - s * s1, s * c1 + c * s1
            for b, value in enumerate(packed_fft(held, 1, swap, sign)):
                shear[b, take, span] = value
        return carry

    lax.fori_loop(0, LANES // TILE, inverse_tile, 0, unroll=2)

    def give(dest):
        return remote(
            shear.at[dest], arrived.at[me], turn_send.at[dest], turn_recv.at[me], dest
        )

    def got(source):
        return remote(
            shear.at[source], arrived.at[source], turn_send.at[source], turn_recv.at[source],
            source,
        )

    def give_plane(plane, begin):
        def give_step(i, carry):
            give(lax.rem(r + i, rows) * planes + plane).start()
            return carry

        lax.fori_loop(begin, rows, give_step, 0)

    give_plane(lax.rem(p + 2, planes), 0)
    give_plane(planes - 1 - p, 0)

    @pl.when(is_end)
    def _():
        lax.fori_loop(1, devices, bins_step, 0)

    give_plane(p + 1 - 2 * lax.rem(p, 2), 0)
    give_plane(p, 1)
    arrived[me] = shear[me]

    def bins_wait(step, carry):
        recv_bins(step).wait_recv()
        return carry

    lax.fori_loop(1, devices, bins_wait, 0)

    order = 4 * (at_row // 8) + lax.rem(at_row, 4)
    swapped = jnp.where(k_me == 0, 0, h_me)
    plain = lax.rem(1 - order // HALF + swapped, 2)
    origin = jnp.where((k_me == 0) & (h_me == 0), 2 * HALF, 2 * HALF - 1)
    inside = lax.rem(order, HALF)
    target = jnp.where(plain == 1, inside, HALF + lax.rem(origin - inside, HALF))
    target = target + which_row * LANES
    table[...] = jnp.where(target == at_column, 1.0, 0.0)

    def bins_turn(k, carry):
        block = bins_in[:, k].reshape(2 * LANES, LANES).astype(BF16)
        out = lax.dot_general(
            block, table[...].astype(BF16), (((0,), (0,)), ((), ())),
            preferred_element_type=F32,
        )
        bands[2 * k] = out[:, :LANES]
        bands[2 * k + 1] = out[:, LANES:]
        return carry

    lax.fori_loop(0, fold // 2, bins_turn, 0, unroll=2)
    sums[...] = jnp.zeros_like(sums)

    def band_step(k, carry):
        flipped = jnp.dot(
            reverse_of(jnp.where(k == 0, 0, 1)), bands[lax.rem(fold - k, fold)].astype(BF16),
            preferred_element_type=F32,
        )
        band = jnp.where(lane < HALF, bands[k], flipped)
        energy = power[k]
        for b in range(NBINS):
            kept = jnp.where(band == float(b), energy, 0.0)
            sums[b] += jnp.sum(kept.reshape(LANES // TILE, TILE, LANES), axis=0)
        return carry

    lax.fori_loop(0, fold, band_step, 0)
    totals = jnp.sum(jnp.sum(sums[...], axis=1), axis=1, keepdims=True)
    diagonal = lax.broadcasted_iota(jnp.int32, (NBINS, LANES), 0) == lax.broadcasted_iota(
        jnp.int32, (NBINS, LANES), 1
    )
    line = jnp.sum(jnp.where(diagonal, totals, 0.0), axis=0, keepdims=True)
    sums_out[...] = jnp.broadcast_to(line, (TILE, LANES))
    sums_in[me] = jnp.broadcast_to(line, (TILE, LANES))

    def tell(step):
        dest = lax.rem(me + step, devices)
        return remote(sums_out, sums_in.at[me], total_send.at[step], total_recv.at[step], dest)

    def told(step):
        source = lax.rem(me + devices - step, devices)
        return remote(
            sums_out, sums_in.at[source], total_send.at[step], total_recv.at[step], source
        )

    def tell_step(step, carry):
        tell(step).start()
        return carry

    lax.fori_loop(1, devices, tell_step, 0)

    def back_step(i, carry):
        near = lax.rem(side_plane + i // rows, pairs)
        k = lax.rem(r + 2 * rows - i, rows) * pairs + near
        for h in range(2):
            @pl.when(2 * k + h != me)
            def _():
                got(2 * k + h).wait_recv()

        angle = (lane * k).astype(F32) * angle_unit
        c, s = jnp.cos(angle), jnp.sin(angle)
        cos, sin = back_base[:, :LANES], back_base[:, LANES:]
        table[:, :LANES] = cos * c - sin * s
        table[:, LANES:] = sin * c + cos * s

        @pl.when(k == 0)
        def _():
            table[...] = back_zero[...]

        left = [
            jnp.concatenate(
                [arrived[2 * k + h, :, part * LANES:(part + 1) * LANES] for h in range(2)], 1
            )
            for part in range(2)
        ]
        folded[k, :2 * LANES] = dot3(jnp.concatenate(left, 0), table[...])
        return carry

    lax.fori_loop(0, slots, back_step, 0, unroll=2)

    for part, out in enumerate((out_real, out_imag)):
        def back_tile(i, carry, part=part, out=out):
            take = pl.ds(pl.multiple_of(part * LANES + i * TILE, TILE), TILE)
            spec = [(folded[0, take, :LANES], None)]
            for k in range(1, slots):
                spec.append((folded[k, take, :LANES], folded[k, take, LANES:]))
            spec.append((folded[0, take, LANES:], None))
            put = pl.ds(pl.multiple_of(i * TILE, TILE), TILE)
            for b, value in enumerate(real_inverse(spec, fold)):
                out[put, b * LANES:(b + 1) * LANES] = value
            return carry

        lax.fori_loop(0, LANES // TILE, back_tile, 0, unroll=2)

    def told_step(step, carry):
        told(step).wait_recv()
        return carry

    lax.fori_loop(1, devices, told_step, 0)
    out_spectrum[...] = jnp.sum(sums_in[...], axis=0)

    def last_step(step, carry):
        give(lax.rem(me + step, devices)).wait_send()
        tell(step).wait_send()
        send_bins(step).wait_send()
        return carry

    lax.fori_loop(1, devices, last_step, 0)

    def sent_step(dest, carry):
        @pl.when(is_end)
        def _():
            for which in (0, 1, 2):
                sum_copy(which, dest).wait_send()

        @pl.when(is_middle)
        def _():
            for which in (3, 4, 5):
                sum_copy(which, dest).wait_send()

        @pl.when(dest != r)
        def _():
            cross(dest).wait_send()

        return carry

    lax.fori_loop(0, rows, sent_step, 0)


def folded_device(density, lens_weight, spectrum_bin):
    rows, planes = lax.axis_size("rows"), lax.axis_size("planes")
    devices = rows * planes
    slab, length = density.shape[1:]
    fold, blocks, slots = devices, slab // LANES, devices // 2
    row_base, row_zero = row_tables(fold)
    back_base, back_zero = back_tables(fold)
    vmem = pl.BlockSpec(memory_space=pltpu.VMEM)
    hbm = pl.BlockSpec(memory_space=pl.ANY)
    smem = pl.BlockSpec(memory_space=pltpu.SMEM)
    dma = pltpu.SemaphoreType.DMA
    chunk = (blocks, LANES, LANES)
    scratch = [
        pltpu.VMEM((2, min(64, slab), length), F32),
        pltpu.VMEM((slots, slab, 2 * LANES), F32),
        pltpu.VMEM((rows, planes) + chunk, F32),
        pltpu.VMEM((rows,) + chunk, F32),
        pltpu.VMEM((rows,) + chunk, F32),
        pltpu.VMEM((rows,) + chunk, F32),
        pltpu.VMEM((rows,) + chunk, F32),
        pltpu.VMEM((rows,) + chunk, F32),
        pltpu.VMEM((fold, LANES, LANES), F32),
        pltpu.VMEM((fold, LANES, LANES), F32),
        pltpu.VMEM((fold, LANES, 2 * LANES), F32),
        pltpu.VMEM((fold, LANES, LANES), F32),
        pltpu.VMEM((devices, LANES, 2 * LANES), F32),
        pltpu.VMEM((length, LANES), jnp.int32),
        pltpu.VMEM((fold, fold // 2, TILE, LANES), F32),
        pltpu.VMEM((devices, fold // 2, TILE, LANES), F32),
        pltpu.VMEM((fold, LANES, LANES), F32),
        pltpu.VMEM((NBINS, TILE, LANES), F32),
        pltpu.VMEM((TILE, LANES), F32),
        pltpu.VMEM((devices, TILE, LANES), F32),
        pltpu.VMEM((2 * LANES, 2 * LANES), F32),
        pltpu.VMEM((LANES, 6 * LANES), BF16),
        dma((2,)),
        dma((6, rows)), dma((6, rows)),
        dma((rows,)), dma((rows,)),
        dma((devices,)), dma((devices,)), dma,
        dma((devices,)), dma((devices,)),
        dma((devices,)), dma((devices,)),
    ]
    real, imag, spectrum = pl.pallas_call(
        functools.partial(shear_kernel, rows, planes, slab),
        out_shape=(
            jax.ShapeDtypeStruct((length // devices, length), F32),
            jax.ShapeDtypeStruct((length // devices, length), F32),
            jax.ShapeDtypeStruct((TILE, LANES), F32),
        ),
        in_specs=[hbm, smem, hbm] + [vmem] * 6,
        out_specs=(vmem, vmem, vmem),
        scratch_shapes=scratch,
        compiler_params=pltpu.CompilerParams(
            collective_id=0, has_side_effects=True, vmem_limit_bytes=67043328
        ),
        name="shear",
    )(
        density[0], lens_weight, spectrum_bin,
        row_base, row_zero, back_base, back_zero, column_table(), turn_table(length),
    )
    return real, imag, spectrum[0, :NBINS]


def phase(left, right, length, orient):
    index = np.arange(left)[:, None] * np.arange(right)[None, :] % length
    return np.exp(orient * 2j * math.pi * index / length)


def as_blocks(table):
    rows = np.stack([table.real, -table.imag], -1), np.stack([table.imag, table.real], -1)
    return np.stack(rows, 1).astype(np.float32)


def lane_table(table):
    top = np.concatenate([table.real, table.imag], 1)
    bottom = np.concatenate([-table.imag, table.real], 1)
    return np.concatenate([top, bottom], 0).astype(np.float32)


def product(pattern, left, right):
    return jnp.einsum(pattern, left, right, precision=lax.Precision.HIGH)


def turn(real, imag, table):
    cos, sin = table.real.astype(np.float32), table.imag.astype(np.float32)
    return real * cos - imag * sin, real * sin + imag * cos


def centred(indices, length):
    return ((indices + length // 2) % length - length // 2).astype(jnp.float32)


def plane_sum(density, lens_weight):
    count = lax.axis_size("planes")
    here = lax.axis_index("planes")
    block = density.shape[1] // count
    half = block // 2

    def own(owner, part):
        start = (owner % count) * block + part * half
        piece = lax.dynamic_slice_in_dim(density, start, half, axis=1)
        return jnp.sum(piece * lens_weight[:, None, None], axis=0)

    ways = ((0, 1), (1, -1))
    held = [own(here - way + count, part) for part, way in ways]
    for step in range(count - 1):
        moved = [
            lax.ppermute(held[part], "planes", [(i, (i + way) % count) for i in range(count)])
            for part, way in ways
        ]
        held = [
            moved[part] + own(here - way * (2 + step) + 2 * count, part) for part, way in ways
        ]
    return jnp.concatenate(held, axis=0)


def on_device(density, lens_weight, spectrum_bin):
    length = density.shape[-1]
    devices = lax.axis_size("rows") * lax.axis_size("planes")
    narrow = length // devices
    me = lax.axis_index("rows") * lax.axis_size("planes") + lax.axis_index("planes")

    share = plane_sum(density, lens_weight)
    field = share.T.reshape(narrow, devices, narrow)
    first = phase(narrow, narrow, narrow, -1)
    real = product("kn,nqy->kqy", first.real.astype(np.float32), field)
    imag = product("kn,nqy->kqy", first.imag.astype(np.float32), field)
    real, imag = turn(real, imag, phase(narrow, devices, length, -1)[:, :, None])
    forward = as_blocks(phase(devices, devices, devices, -1))
    spread = product("leq,kqy->leky", forward[..., 0], real) + product(
        "leq,kqy->leky", forward[..., 1], imag
    )
    held = lax.all_to_all(spread, AXES, split_axis=0, concat_axis=0, tiled=True)

    held = product("kesc,scxt->kext", forward, held)
    real, imag = turn(held[:, 0], held[:, 1], phase(devices, narrow, length, -1)[:, None, :])
    hat = product(
        "kxt,tm->kxm",
        jnp.concatenate([real, imag], -1),
        lane_table(phase(narrow, narrow, narrow, -1)),
    )
    hat_real, hat_imag = hat[..., :narrow], hat[..., narrow:]

    ky_index = (
        jnp.arange(devices, dtype=jnp.int32)[:, None, None]
        + devices * jnp.arange(narrow, dtype=jnp.int32)[None, None, :]
    )
    height = centred(ky_index, length)
    across = centred(me * narrow + jnp.arange(narrow, dtype=jnp.int32), length)[None, :, None]
    square_norm = height**2 + across**2
    anchor = square_norm == 0
    safe_norm = jnp.where(anchor, 1.0, square_norm)
    hat_real = jnp.where(anchor, 0.0, hat_real)
    hat_imag = jnp.where(anchor, 0.0, hat_imag)

    kernel_real = (across**2 - height**2) / safe_norm
    kernel_imag = 2.0 * across * height / safe_norm
    shear = jnp.concatenate(
        [
            kernel_real * hat_real - kernel_imag * hat_imag,
            kernel_real * hat_imag + kernel_imag * hat_real,
        ],
        -1,
    )
    back = product(
        "kxm,mt->kxt", shear, lane_table(phase(narrow, narrow, narrow, 1) / length)
    )
    real, imag = turn(
        back[..., :narrow], back[..., narrow:], phase(devices, narrow, length, 1)[:, None, :]
    )
    inverse = as_blocks(phase(devices, devices, devices, 1))
    back = product("sek,kxt->sext", inverse[..., 0], real) + product(
        "sek,kxt->sext", inverse[..., 1], imag
    )
    turned = lax.all_to_all(back, AXES, split_axis=0, concat_axis=0, tiled=True)

    pixel_power = (hat_real**2 + hat_imag**2) * (NBINS / float(length) ** 4)
    bins = spectrum_bin.reshape(narrow, devices, narrow).transpose(1, 2, 0)
    band_ids = jnp.arange(NBINS, dtype=jnp.int32)[:, None, None, None]
    partial_power = jnp.sum(jnp.where(bins == band_ids, pixel_power, 0.0), axis=(1, 2, 3))
    copies = jnp.broadcast_to(partial_power, (devices, 8, NBINS))
    gathered = lax.all_to_all(copies, AXES, split_axis=0, concat_axis=0, tiled=True)
    spectrum = jnp.sum(gathered[:, 0, :], axis=0)

    turned = product("aedc,dcqt->aeqt", inverse, turned)
    real, imag = turn(
        turned[:, 0], turned[:, 1], phase(devices, narrow, length, 1)[:, :, None]
    )
    last = phase(narrow, narrow, narrow, 1) / length
    cos, sin = last.real.astype(np.float32), last.imag.astype(np.float32)
    out_real = product("bq,aqt->bat", cos, real) - product("bq,aqt->bat", sin, imag)
    out_imag = product("bq,aqt->bat", sin, real) + product("bq,aqt->bat", cos, imag)
    shape = (length, narrow)
    return (out_real.reshape(shape).T, out_imag.reshape(shape).T, spectrum)


def folds(mesh, density):
    rows, planes = mesh.shape["rows"], mesh.shape["planes"]
    count, length, width = density.shape
    return (
        count == planes
        and planes == 4
        and length == width == LANES * rows * planes
        and rows * planes == LANES // 4
    )


def solution(mesh):
    specs = (P("planes", "rows", None), P("planes"), P(None, AXES))
    outs = (P(AXES, None), P(AXES, None), P())

    def run(density, lens_weight, spectrum_bin):
        if folds(mesh, density):
            body = folded_device
        else:
            body = on_device
        whole = jax.shard_map(body, mesh=mesh, in_specs=specs, out_specs=outs, check_vma=False)
        return whole(density, lens_weight, spectrum_bin)

    return run
```

```python
import functools
import math

import jax
import jax.numpy as jnp
import numpy as np
from jax import lax
from jax.experimental import pallas as pl
from jax.experimental.pallas import tpu as pltpu
from jax.sharding import PartitionSpec as P

NBINS = 64
AXES = ("rows", "planes")
LANES = 128
HALF = LANES // 2
TILE = 8
MESH = pl.DeviceIdType.MESH
F32 = jnp.float32
BF16 = jnp.bfloat16


def real_fft(xs):
    n = len(xs)
    if n == 2:
        return [(xs[0] + xs[1], None), (xs[0] - xs[1], None)]
    even, odd = real_fft(xs[0::2]), real_fft(xs[1::2])
    out = [None] * (n // 2 + 1)
    out[0] = (even[0][0] + odd[0][0], None)
    out[n // 2] = (even[0][0] - odd[0][0], None)
    out[n // 4] = (even[n // 4][0], -odd[n // 4][0])
    for k in range(1, n // 4):
        c, s = math.cos(2 * math.pi * k / n), math.sin(2 * math.pi * k / n)
        (er, ei), (odr, odi) = even[k], odd[k]
        tr, ti = c * odr + s * odi, c * odi - s * odr
        out[k] = (er + tr, ei + ti)
        out[n // 2 - k] = (er - tr, ti - ei)
    return out


def real_inverse(spec, n):
    if n == 2:
        return [spec[0][0] + spec[1][0], spec[0][0] - spec[1][0]]
    h, q = n // 2, n // 4
    even, odd = [None] * (q + 1), [None] * (q + 1)
    even[0] = (spec[0][0] + spec[h][0], None)
    odd[0] = (spec[0][0] - spec[h][0], None)
    even[q] = (2.0 * spec[q][0], None)
    odd[q] = (-2.0 * spec[q][1], None)
    for k in range(1, q):
        (ar, ai), (br, bi) = spec[k], spec[h - k]
        even[k] = (ar + br, ai - bi)
        ur, ui = ar - br, ai + bi
        c, s = math.cos(2 * math.pi * k / n), math.sin(2 * math.pi * k / n)
        odd[k] = (c * ur - s * ui, c * ui + s * ur)
    evens, odds = real_inverse(even, h), real_inverse(odd, h)
    out = [None] * n
    out[0::2], out[1::2] = evens, odds
    return out


def packed_fft(xs, orient, swap, sign):
    n = len(xs)
    if n == 1:
        return xs
    even = packed_fft(xs[0::2], orient, swap, sign)
    odd = packed_fft(xs[1::2], orient, swap, sign)
    out = [None] * n
    for k in range(n // 2):
        c, s = math.cos(2 * math.pi * k / n), orient * math.sin(2 * math.pi * k / n)
        if k == 0:
            t = odd[0]
        elif 4 * k == n:
            t = swap(odd[k]) * (orient * sign)
        else:
            t = c * odd[k] + swap(odd[k]) * (s * sign)
        out[k], out[k + n // 2] = even[k] + t, even[k] - t
    return out


def split(x):
    high = x.astype(BF16)
    return high, (x - high.astype(F32)).astype(BF16)


def dot3(left, right):
    lh, ll = split(left)
    rh, rl = split(right)
    return jnp.dot(
        jnp.concatenate([lh, lh, ll], 1),
        jnp.concatenate([rh, rl, rh], 0),
        preferred_element_type=F32,
    )


def row_tables(fold):
    length = fold * LANES
    a = np.arange(LANES)
    general = np.zeros((2, LANES, 2, 2, HALF))
    special = np.zeros((2, LANES, 2, 2, HALF))
    for h in range(2):
        m = h * HALF + np.arange(HALF)
        angle = 2 * np.pi * (a[:, None] * m[None, :] % LANES) / LANES
        general[0, :, h, 0], general[0, :, h, 1] = np.cos(angle), -np.sin(angle)
        general[1, :, h, 0], general[1, :, h, 1] = np.sin(angle), np.cos(angle)
        kx = fold * np.arange(HALF) + h * (fold // 2)
        angle = 2 * np.pi * (a[:, None] * kx[None, :] % length) / length
        special[h, :, h, 0], special[h, :, h, 1] = np.cos(angle), -np.sin(angle)
    special[0, :, 0, 1, 0] = 1 - 2 * (a % 2)
    shape = (2 * LANES, 2 * LANES)
    return general.reshape(shape).astype(np.float32), special.reshape(shape).astype(np.float32)


def back_tables(fold):
    length = fold * LANES
    a = np.arange(LANES)
    general = np.zeros((2, 2, HALF, 2, LANES))
    special = np.zeros((2, 2, HALF, 2, LANES))
    for h in range(2):
        m = h * HALF + np.arange(HALF)
        angle = 2 * np.pi * (m[:, None] * a[None, :] % LANES) / LANES
        general[h, 0, :, 0], general[h, 0, :, 1] = np.cos(angle), np.sin(angle)
        general[h, 1, :, 0], general[h, 1, :, 1] = -np.sin(angle), np.cos(angle)
        kx = fold * np.arange(HALF) + h * (fold // 2)
        angle = 2 * np.pi * (kx[:, None] * a[None, :] % length) / length
        special[h, 0, :, h], special[h, 1, :, h] = 2 * np.cos(angle), -2 * np.sin(angle)
    special[0, 0, 0, 0] = 1.0
    special[0, 1, 0, 0] = 1 - 2 * (a % 2)
    shape, scale = (2 * LANES, 2 * LANES), float(length) ** -2
    return (
        (general.reshape(shape) * scale).astype(np.float32),
        (special.reshape(shape) * scale).astype(np.float32),
    )


def column_table():
    a = np.arange(LANES)
    angle = 2 * np.pi * (a[:, None] * a[None, :] % LANES) / LANES
    return np.concatenate([np.cos(angle), np.sin(angle)], 1).astype(np.float32)


def turn_table(length):
    angle = 2 * np.pi * np.arange(LANES)[:, None] / length * np.ones((1, LANES))
    return np.stack([np.cos(angle), np.sin(angle)]).astype(np.float32)


def shear_kernel(
    rows, planes, slab,
    density, weight, bins, row_base, row_zero, back_base, back_zero, column, turns,
    out_real, out_imag, out_spectrum,
    staged, folded, parts, outer_inner, outer_own, outer_far, inner_outer, last_own, lines, hat, shear, power,
    arrived, bins_raw, bins_out, bins_in, bands, sums, sums_out, sums_in, table, split_column,
    stage_sem, sum_send, sum_recv, cross_send, cross_recv,
    bins_send, bins_recv, bins_load, turn_send, turn_recv, total_send, total_recv,
):
    devices = rows * planes
    fold = devices
    length = fold * LANES
    slots = fold // 2
    blocks = slab // LANES
    pairs = planes // 2
    angle_unit = 2 * math.pi / length
    r, p = lax.axis_index("rows"), lax.axis_index("planes")
    me = r * planes + p

    def place(device):
        return {"rows": device // planes, "planes": lax.rem(device, planes)}

    def remote(source, target, send, recv, device):
        return pltpu.make_async_remote_copy(
            source, target, send, recv, device_id=place(device), device_id_type=MESH
        )

    lane = lax.broadcasted_iota(jnp.int32, (1, LANES), 1)
    sign = jnp.where(lane < HALF, -1.0, 1.0)

    def swap(x):
        return pltpu.roll(x, HALF, axis=1)

    def times_i(x):
        return swap(x) * sign

    def minus_i(x):
        return swap(x) * (-sign)

    barrier = pltpu.get_barrier_semaphore()
    for step in range(1, devices):
        pl.semaphore_signal(
            barrier, inc=1, device_id=place(lax.rem(me + step, devices)), device_id_type=MESH
        )
    load_bins = pltpu.make_async_copy(bins, bins_raw, bins_load)
    load_bins.start()

    depth = staged.shape[1]
    chunks = slab // depth

    def stage(c):
        slot = lax.rem(c, 2)
        return pltpu.make_async_copy(
            density.at[pl.ds(c * depth, depth)], staged.at[slot], stage_sem.at[slot]
        )

    stage(0).start()
    scale = weight[0]

    def stage_step(c, carry):
        @pl.when(c + 1 < chunks)
        def _():
            stage(c + 1).start()

        stage(c).wait()
        slot = lax.rem(c, 2)

        def tile(i, carry):
            take = pl.ds(pl.multiple_of(i * TILE, TILE), TILE)
            xs = [staged[slot, take, b * LANES:(b + 1) * LANES] * scale for b in range(fold)]
            spec = real_fft(xs)
            put = pl.ds(pl.multiple_of(c * depth + i * TILE, TILE), TILE)
            folded[0, put, :LANES] = spec[0][0]
            folded[0, put, LANES:] = spec[slots][0]
            for k in range(1, slots):
                folded[k, put, :LANES] = spec[k][0]
                folded[k, put, LANES:] = spec[k][1]
            return carry

        return lax.fori_loop(0, depth // TILE, tile, carry, unroll=2)

    lax.fori_loop(0, chunks, stage_step, 0)

    side_plane = p // 2
    end, centre = (planes - 1) * side_plane, 1 + side_plane
    inner = planes - 1 - p
    is_end = lax.rem(p, planes - 1) == 0
    is_middle = lax.rem(p, planes - 1) > 0

    def sum_copy(which, dest):
        owner, target, to = (
            (planes - 1 - centre, outer_inner, centre),
            (centre, outer_own, centre),
            (planes - 1 - p, outer_far, centre),
            (inner, last_own, inner),
            (planes - 1 - end, inner_outer, inner),
            (end, last_own, end),
        )[which]
        return remote(
            parts.at[dest, owner], target.at[dest],
            sum_send.at[which, dest], sum_recv.at[which, dest], r * planes + to,
        )

    def sum_wait(which, dest):
        target = (outer_inner, outer_own, outer_far, last_own, inner_outer, last_own)[which]
        remote(
            target.at[dest], target.at[dest], sum_send.at[which, dest],
            sum_recv.at[which, dest], r * planes + lax.rem(p + 1, planes),
        ).wait_recv()

    def cross(dest):
        return remote(
            parts.at[dest, p], lines.at[pl.ds(r * blocks, blocks)],
            cross_send.at[dest], cross_recv.at[r], dest * planes + p,
        )

    def crossed(source):
        return remote(
            parts.at[source, p], lines.at[pl.ds(source * blocks, blocks)],
            cross_send.at[source], cross_recv.at[source], source * planes + p,
        )

    at_a = lax.broadcasted_iota(jnp.int32, (LANES, LANES), 0)

    def row_products(i):
        dest = lax.rem(r + 1 + i, rows)
        for pair in range(pairs):
            k = dest * pairs + pair
            angle = (at_a * k).astype(F32) * angle_unit
            c, s = jnp.cos(angle), jnp.sin(angle)
            c, s = jnp.concatenate([c, c], 1), jnp.concatenate([s, s], 1)
            top, low = row_base[:LANES], row_base[LANES:]
            table[:LANES] = c * top - s * low
            table[LANES:] = c * low + s * top

            @pl.when(k == 0)
            def _():
                table[...] = row_zero[...]

            right = table[...]
            for q in range(blocks):
                done = dot3(folded[k, q * LANES:(q + 1) * LANES], right)
                parts[dest, 2 * pair, q] = done[:, :LANES]
                parts[dest, 2 * pair + 1, q] = done[:, LANES:]


    def turn_of(i):
        return lax.rem(r + 1 + i, rows)

    def row_step(i, carry):
        @pl.when(is_end)
        def _():
            sum_copy(2, turn_of(i)).start()

        @pl.when(i + 1 < rows)
        def _():
            row_products(i + 1)

        return carry

    row_products(jnp.int32(0))
    pl.semaphore_wait(barrier, devices - 1)
    lax.fori_loop(0, rows, row_step, 0)

    @pl.when(is_end)
    def _():
        def near_step(i, carry):
            sum_copy(0, turn_of(i)).start()
            sum_copy(1, turn_of(i)).start()
            return carry

        lax.fori_loop(0, rows, near_step, 0)

    at_row = lax.broadcasted_iota(jnp.int32, (2 * LANES, 2 * LANES), 0)
    at_column = lax.broadcasted_iota(jnp.int32, (2 * LANES, 2 * LANES), 1)
    which_row = lax.rem(at_row // 4, 2)
    target = which_row * LANES + lax.rem(at_row, 4) * fold + at_row // 8
    table[...] = jnp.where(target == at_column, 1.0, 0.0)
    load_bins.wait()

    def bins_layout(k, carry):
        both = [bins_raw[pl.ds(2 * k + q, LANES, stride=fold), :] for q in range(2)]
        both = jnp.concatenate(both, 1).astype(F32).astype(BF16)
        out = lax.dot_general(
            table[...].astype(BF16), both, (((1,), (1,)), ((), ())), preferred_element_type=F32
        )
        bins_out[:, k] = out.reshape(fold, TILE, LANES)
        return carry

    lax.fori_loop(0, fold // 2, bins_layout, 0, unroll=2)
    side = me // slots

    def class_at(owner):
        k, h = owner // 2, lax.rem(owner, 2)
        other = k + lax.rem(h + side, 2) * (fold - 2 * k)
        return jnp.where(k == 0, h * slots, other)

    def send_bins(step):
        owner = lax.rem(me + step, devices)
        return remote(
            bins_out.at[class_at(owner)], bins_in.at[me],
            bins_send.at[step], bins_recv.at[step], owner,
        )

    def recv_bins(step):
        source = lax.rem(me + devices - step, devices)
        return remote(
            bins_out.at[0], bins_in.at[source], bins_send.at[step], bins_recv.at[step], source
        )

    def own_sum(dest):
        @pl.when(dest != r)
        def _():
            cross(dest).start()

    @pl.when(is_middle)
    def _():
        def far_relay(i, carry):
            @pl.when(i < rows)
            def _():
                dest = turn_of(i)
                sum_wait(2, dest)
                owner = planes - 1 - end
                parts[dest, owner] = parts[dest, owner] + outer_far[dest]
                sum_copy(4, dest).start()

            @pl.when(i > 0)
            def _():
                dest = turn_of(i - 1)
                sum_wait(4, dest)
                parts[dest, end] = parts[dest, end] + inner_outer[dest]
                sum_copy(5, dest).start()

            return carry

        lax.fori_loop(0, rows + 1, far_relay, 0)

    def bins_step(step, carry):
        send_bins(step).start()
        return carry

    @pl.when(is_middle)
    def _():
        lax.fori_loop(1, devices, bins_step, 0)

    bins_in[me] = bins_out[class_at(me)]

    @pl.when(is_middle)
    def _():
        def near_relay(i, carry):
            @pl.when(i < rows)
            def _():
                dest = turn_of(i)
                sum_wait(0, dest)
                parts[dest, inner] = parts[dest, inner] + outer_inner[dest]
                sum_copy(3, dest).start()

            @pl.when(i > 1)
            def _():
                dest = turn_of(i - 2)
                sum_wait(1, dest)
                sum_wait(3, dest)
                parts[dest, p] = parts[dest, p] + outer_own[dest] + last_own[dest]
                own_sum(dest)

            return carry

        lax.fori_loop(0, rows + 2, near_relay, 0)

    @pl.when(is_end)
    def _():
        def end_step(i, carry):
            dest = turn_of(i)
            sum_wait(5, dest)
            parts[dest, p] = parts[dest, p] + last_own[dest]
            own_sum(dest)
            return carry

        lax.fori_loop(0, rows, end_step, 0)

    def own_step(q, carry):
        lines[r * blocks + q] = parts[r, p, q]
        return carry

    lax.fori_loop(0, blocks, own_step, 0)

    def crossed_step(i, carry):
        crossed(lax.rem(r + rows - 1 - i, rows)).wait_recv()
        return carry

    lax.fori_loop(0, rows - 1, crossed_step, 0)

    def column_tile(i, carry):
        take = pl.ds(pl.multiple_of(i * TILE, TILE), TILE)
        spec = packed_fft([lines[b, take] for b in range(fold)], -1, swap, sign)
        lines[0, take] = spec[0]
        c1, s1 = turns[0, take], turns[1, take] * sign
        c, s = c1, s1
        for k in range(1, fold):
            lines[k, take] = spec[k] * c - swap(spec[k]) * s
            c, s = c * c1 - s * s1, s * c1 + c * s1
        return carry

    lax.fori_loop(0, LANES // TILE, column_tile, 0, unroll=2)

    k_me, h_me = me // 2, lax.rem(me, 2)
    index = lax.rem(lane, HALF)
    kx = jnp.where(
        k_me == 0, fold * index + h_me * slots, fold * (HALF * h_me + index) + k_me
    )
    across = jnp.where(kx >= length // 2, kx - length, kx).astype(F32)
    my = lax.broadcasted_iota(jnp.int32, (LANES, LANES), 0)
    at_lane = lax.broadcasted_iota(jnp.int32, (LANES, LANES), 1)
    pixel_scale = NBINS / float(length) ** 4

    def height_of(k):
        ky = k + fold * my
        return jnp.where(ky >= length // 2, ky - length, ky).astype(F32)

    def kernel_of(width, height):
        square_norm = height * height + width * width
        safe = jnp.where(square_norm == 0.0, 1.0, square_norm)
        inverse = 1.0 / safe
        return (width * width - height * height) * inverse, 2.0 * width * height * inverse

    def edge_of(k):
        return (my == HALF) & (k == 0)

    high, low = split(column[...])
    split_column[...] = jnp.concatenate([high, high, low], 1)

    def column_product(right):
        rh, rl = split(right)
        return jnp.dot(
            split_column[...], jnp.concatenate([rh, rl, rh], 0), preferred_element_type=F32
        )

    def each(f, x):
        count = x.shape[1] // LANES
        return jnp.concatenate([f(x[:, q * LANES:(q + 1) * LANES]) for q in range(count)], 1)

    def column_step(j, carry):
        z = jnp.concatenate([lines[2 * j], lines[2 * j + 1]], 1)
        both = column_product(jnp.concatenate([z, each(minus_i, z)], 0))
        turned = []
        for q in range(2):
            k = 2 * j + q
            v = both[:, q * LANES:(q + 1) * LANES]
            hat[k] = v
            square = v * v
            power[k] = (square + swap(square)) * pixel_scale
            kernel_real, kernel_imag = kernel_of(across, height_of(k))
            edge = edge_of(k)
            turned += [
                kernel_real * v + jnp.where(edge, kernel_imag * times_i(v), 0.0),
                jnp.where(edge, 0.0, kernel_imag * v),
            ]
        turned = jnp.concatenate(turned, 1)
        back = column_product(jnp.concatenate([turned, each(times_i, turned)], 0))
        shear[2 * j] = back[:, :2 * LANES]
        shear[2 * j + 1] = back[:, 2 * LANES:]
        return carry

    lax.fori_loop(0, fold // 2, column_step, 0, unroll=2)

    def reverse_of(wrap):
        return jnp.where(lax.rem(LANES - wrap - my, LANES) == at_lane, 1.0, 0.0).astype(BF16)

    @pl.when(me == 0)
    def _():
        spot = lax.rem(at_lane, HALF)

        def gather(k, held):
            return jnp.where(spot == k, pltpu.roll(hat[k], k, axis=1), held)

        v = lax.fori_loop(0, fold, gather, jnp.zeros((LANES, LANES), F32), unroll=2)
        high, low = split(v)

        def moved(wrap):
            mover = reverse_of(wrap)
            return jnp.dot(mover, high, preferred_element_type=F32) + jnp.dot(
                mover, low, preferred_element_type=F32
            )

        my_spot = lax.rem(my, HALF)
        same = (my // HALF == at_lane // HALF) & (spot < fold)
        partner = jnp.where(same & (lax.rem(fold - spot, fold) == my_spot), 1.0, 0.0)
        partner = partner.astype(BF16)
        high, low = split(jnp.where(spot == 0, moved(0), moved(1)))
        mirror = jnp.dot(high, partner, preferred_element_type=F32) + jnp.dot(
            low, partner, preferred_element_type=F32
        )
        mirror = mirror * (-sign)
        zero = jnp.where((my == 0) & (spot == 0), 0.0, (v + mirror) * 0.5)
        last = minus_i((v - mirror) * 0.5)
        zero_square, last_square = zero * zero, last * last
        powers = jnp.where(
            at_lane < HALF, zero_square + swap(zero_square), last_square + swap(last_square)
        ) * pixel_scale
        ky = spot + fold * my
        height = jnp.where(ky >= length // 2, ky - length, ky).astype(F32)
        kernel_real, kernel_imag = kernel_of(float(-(length // 2)), height)
        turned = times_i(kernel_real * last + kernel_imag * times_i(last))
        edge = ky == length // 2
        real = jnp.where(edge, 0.0, turned) - zero
        imag = jnp.where(edge, times_i(last), 0.0)
        both = jnp.concatenate([real, imag], 1)
        back = column_product(jnp.concatenate([both, each(times_i, both)], 0))

        def scatter(k, carry):
            shift = lax.rem(LANES - k, LANES)
            for part in range(2):
                span = slice(part * LANES, (part + 1) * LANES)
                value = pltpu.roll(back[:, span], shift, axis=1)
                shear[k, :, span] = jnp.where(spot == 0, value, shear[k, :, span])
            power[k] = jnp.where(spot == 0, pltpu.roll(powers, shift, axis=1), power[k])
            return carry

        lax.fori_loop(0, fold, scatter, 0, unroll=2)

    def inverse_tile(i, carry):
        take = pl.ds(pl.multiple_of(i * TILE, TILE), TILE)
        c1, s1 = turns[0, take], turns[1, take] * sign
        for part in range(2):
            span = slice(part * LANES, (part + 1) * LANES)
            c, s = c1, s1
            held = [shear[0, take, span]]
            for k in range(1, fold):
                value = shear[k, take, span]
                held.append(value * c + swap(value) * s)
                c, s = c * c1 - s * s1, s * c1 + c * s1
            for b, value in enumerate(packed_fft(held, 1, swap, sign)):
                shear[b, take, span] = value
        return carry

    lax.fori_loop(0, LANES // TILE, inverse_tile, 0, unroll=2)

    def give(dest):
        return remote(
            shear.at[dest], arrived.at[me], turn_send.at[dest], turn_recv.at[me], dest
        )

    def got(source):
        return remote(
            shear.at[source], arrived.at[source], turn_send.at[source], turn_recv.at[source],
            source,
        )

    def give_plane(plane, begin):
        def give_step(i, carry):
            give(lax.rem(r + i, rows) * planes + plane).start()
            return carry

        lax.fori_loop(begin, rows, give_step, 0)

    give_plane(lax.rem(p + 2, planes), 0)

    @pl.when(is_end)
    def _():
        lax.fori_loop(1, devices, bins_step, 0)

    give_plane(planes - 1 - p, 0)
    give_plane(p + 1 - 2 * lax.rem(p, 2), 0)
    give_plane(p, 1)
    arrived[me] = shear[me]

    def bins_wait(step, carry):
        recv_bins(step).wait_recv()
        return carry

    lax.fori_loop(1, devices, bins_wait, 0)

    order = 4 * (at_row // 8) + lax.rem(at_row, 4)
    swapped = jnp.where(k_me == 0, 0, h_me)
    plain = lax.rem(1 - order // HALF + swapped, 2)
    origin = jnp.where((k_me == 0) & (h_me == 0), 2 * HALF, 2 * HALF - 1)
    inside = lax.rem(order, HALF)
    target = jnp.where(plain == 1, inside, HALF + lax.rem(origin - inside, HALF))
    target = target + which_row * LANES
    table[...] = jnp.where(target == at_column, 1.0, 0.0)

    def bins_turn(k, carry):
        block = bins_in[:, k].reshape(2 * LANES, LANES).astype(BF16)
        out = lax.dot_general(
            block, table[...].astype(BF16), (((0,), (0,)), ((), ())),
            preferred_element_type=F32,
        )
        bands[2 * k] = out[:, :LANES]
        bands[2 * k + 1] = out[:, LANES:]
        return carry

    lax.fori_loop(0, fold // 2, bins_turn, 0, unroll=2)
    sums[...] = jnp.zeros_like(sums)

    def band_step(k, carry):
        flipped = jnp.dot(
            reverse_of(jnp.where(k == 0, 0, 1)), bands[lax.rem(fold - k, fold)].astype(BF16),
            preferred_element_type=F32,
        )
        band = jnp.where(lane < HALF, bands[k], flipped)
        energy = power[k]
        for b in range(NBINS):
            kept = jnp.where(band == float(b), energy, 0.0)
            sums[b] += jnp.sum(kept.reshape(LANES // TILE, TILE, LANES), axis=0)
        return carry

    lax.fori_loop(0, fold, band_step, 0)
    totals = jnp.sum(jnp.sum(sums[...], axis=1), axis=1, keepdims=True)
    diagonal = lax.broadcasted_iota(jnp.int32, (NBINS, LANES), 0) == lax.broadcasted_iota(
        jnp.int32, (NBINS, LANES), 1
    )
    line = jnp.sum(jnp.where(diagonal, totals, 0.0), axis=0, keepdims=True)
    sums_out[...] = jnp.broadcast_to(line, (TILE, LANES))
    sums_in[me] = jnp.broadcast_to(line, (TILE, LANES))

    def tell(step):
        dest = lax.rem(me + step, devices)
        return remote(sums_out, sums_in.at[me], total_send.at[step], total_recv.at[step], dest)

    def told(step):
        source = lax.rem(me + devices - step, devices)
        return remote(
            sums_out, sums_in.at[source], total_send.at[step], total_recv.at[step], source
        )

    def tell_step(step, carry):
        tell(step).start()
        return carry

    lax.fori_loop(1, devices, tell_step, 0)

    def back_step(i, carry):
        near = lax.rem(side_plane + i // rows, pairs)
        k = lax.rem(r + 2 * rows - i, rows) * pairs + near
        for h in range(2):
            @pl.when(2 * k + h != me)
            def _():
                got(2 * k + h).wait_recv()

        angle = (lane * k).astype(F32) * angle_unit
        c, s = jnp.cos(angle), jnp.sin(angle)
        cos, sin = back_base[:, :LANES], back_base[:, LANES:]
        table[:, :LANES] = cos * c - sin * s
        table[:, LANES:] = sin * c + cos * s

        @pl.when(k == 0)
        def _():
            table[...] = back_zero[...]

        left = [
            jnp.concatenate(
                [arrived[2 * k + h, :, part * LANES:(part + 1) * LANES] for h in range(2)], 1
            )
            for part in range(2)
        ]
        folded[k, :2 * LANES] = dot3(jnp.concatenate(left, 0), table[...])
        return carry

    lax.fori_loop(0, slots, back_step, 0, unroll=2)

    for part, out in enumerate((out_real, out_imag)):
        def back_tile(i, carry, part=part, out=out):
            take = pl.ds(pl.multiple_of(part * LANES + i * TILE, TILE), TILE)
            spec = [(folded[0, take, :LANES], None)]
            for k in range(1, slots):
                spec.append((folded[k, take, :LANES], folded[k, take, LANES:]))
            spec.append((folded[0, take, LANES:], None))
            put = pl.ds(pl.multiple_of(i * TILE, TILE), TILE)
            for b, value in enumerate(real_inverse(spec, fold)):
                out[put, b * LANES:(b + 1) * LANES] = value
            return carry

        lax.fori_loop(0, LANES // TILE, back_tile, 0, unroll=2)

    def told_step(step, carry):
        told(step).wait_recv()
        return carry

    lax.fori_loop(1, devices, told_step, 0)
    out_spectrum[...] = jnp.sum(sums_in[...], axis=0)

    def last_step(step, carry):
        give(lax.rem(me + step, devices)).wait_send()
        tell(step).wait_send()
        send_bins(step).wait_send()
        return carry

    lax.fori_loop(1, devices, last_step, 0)

    def sent_step(dest, carry):
        @pl.when(is_end)
        def _():
            for which in (0, 1, 2):
                sum_copy(which, dest).wait_send()

        @pl.when(is_middle)
        def _():
            for which in (3, 4, 5):
                sum_copy(which, dest).wait_send()

        @pl.when(dest != r)
        def _():
            cross(dest).wait_send()

        return carry

    lax.fori_loop(0, rows, sent_step, 0)


def folded_device(density, lens_weight, spectrum_bin):
    rows, planes = lax.axis_size("rows"), lax.axis_size("planes")
    devices = rows * planes
    slab, length = density.shape[1:]
    fold, blocks, slots = devices, slab // LANES, devices // 2
    row_base, row_zero = row_tables(fold)
    back_base, back_zero = back_tables(fold)
    vmem = pl.BlockSpec(memory_space=pltpu.VMEM)
    hbm = pl.BlockSpec(memory_space=pl.ANY)
    smem = pl.BlockSpec(memory_space=pltpu.SMEM)
    dma = pltpu.SemaphoreType.DMA
    chunk = (blocks, LANES, LANES)
    scratch = [
        pltpu.VMEM((2, min(64, slab), length), F32),
        pltpu.VMEM((slots, slab, 2 * LANES), F32),
        pltpu.VMEM((rows, planes) + chunk, F32),
        pltpu.VMEM((rows,) + chunk, F32),
        pltpu.VMEM((rows,) + chunk, F32),
        pltpu.VMEM((rows,) + chunk, F32),
        pltpu.VMEM((rows,) + chunk, F32),
        pltpu.VMEM((rows,) + chunk, F32),
        pltpu.VMEM((fold, LANES, LANES), F32),
        pltpu.VMEM((fold, LANES, LANES), F32),
        pltpu.VMEM((fold, LANES, 2 * LANES), F32),
        pltpu.VMEM((fold, LANES, LANES), F32),
        pltpu.VMEM((devices, LANES, 2 * LANES), F32),
        pltpu.VMEM((length, LANES), jnp.int32),
        pltpu.VMEM((fold, fold // 2, TILE, LANES), F32),
        pltpu.VMEM((devices, fold // 2, TILE, LANES), F32),
        pltpu.VMEM((fold, LANES, LANES), F32),
        pltpu.VMEM((NBINS, TILE, LANES), F32),
        pltpu.VMEM((TILE, LANES), F32),
        pltpu.VMEM((devices, TILE, LANES), F32),
        pltpu.VMEM((2 * LANES, 2 * LANES), F32),
        pltpu.VMEM((LANES, 6 * LANES), BF16),
        dma((2,)),
        dma((6, rows)), dma((6, rows)),
        dma((rows,)), dma((rows,)),
        dma((devices,)), dma((devices,)), dma,
        dma((devices,)), dma((devices,)),
        dma((devices,)), dma((devices,)),
    ]
    real, imag, spectrum = pl.pallas_call(
        functools.partial(shear_kernel, rows, planes, slab),
        out_shape=(
            jax.ShapeDtypeStruct((length // devices, length), F32),
            jax.ShapeDtypeStruct((length // devices, length), F32),
            jax.ShapeDtypeStruct((TILE, LANES), F32),
        ),
        in_specs=[hbm, smem, hbm] + [vmem] * 6,
        out_specs=(vmem, vmem, vmem),
        scratch_shapes=scratch,
        compiler_params=pltpu.CompilerParams(
            collective_id=0, has_side_effects=True, vmem_limit_bytes=67043328
        ),
        name="shear",
    )(
        density[0], lens_weight, spectrum_bin,
        row_base, row_zero, back_base, back_zero, column_table(), turn_table(length),
    )
    return real, imag, spectrum[0, :NBINS]


def phase(left, right, length, orient):
    index = np.arange(left)[:, None] * np.arange(right)[None, :] % length
    return np.exp(orient * 2j * math.pi * index / length)


def as_blocks(table):
    rows = np.stack([table.real, -table.imag], -1), np.stack([table.imag, table.real], -1)
    return np.stack(rows, 1).astype(np.float32)


def lane_table(table):
    top = np.concatenate([table.real, table.imag], 1)
    bottom = np.concatenate([-table.imag, table.real], 1)
    return np.concatenate([top, bottom], 0).astype(np.float32)


def product(pattern, left, right):
    return jnp.einsum(pattern, left, right, precision=lax.Precision.HIGH)


def turn(real, imag, table):
    cos, sin = table.real.astype(np.float32), table.imag.astype(np.float32)
    return real * cos - imag * sin, real * sin + imag * cos


def centred(indices, length):
    return ((indices + length // 2) % length - length // 2).astype(jnp.float32)


def plane_sum(density, lens_weight):
    count = lax.axis_size("planes")
    here = lax.axis_index("planes")
    block = density.shape[1] // count
    half = block // 2

    def own(owner, part):
        start = (owner % count) * block + part * half
        piece = lax.dynamic_slice_in_dim(density, start, half, axis=1)
        return jnp.sum(piece * lens_weight[:, None, None], axis=0)

    ways = ((0, 1), (1, -1))
    held = [own(here - way + count, part) for part, way in ways]
    for step in range(count - 1):
        moved = [
            lax.ppermute(held[part], "planes", [(i, (i + way) % count) for i in range(count)])
            for part, way in ways
        ]
        held = [
            moved[part] + own(here - way * (2 + step) + 2 * count, part) for part, way in ways
        ]
    return jnp.concatenate(held, axis=0)


def on_device(density, lens_weight, spectrum_bin):
    length = density.shape[-1]
    devices = lax.axis_size("rows") * lax.axis_size("planes")
    narrow = length // devices
    me = lax.axis_index("rows") * lax.axis_size("planes") + lax.axis_index("planes")

    share = plane_sum(density, lens_weight)
    field = share.T.reshape(narrow, devices, narrow)
    first = phase(narrow, narrow, narrow, -1)
    real = product("kn,nqy->kqy", first.real.astype(np.float32), field)
    imag = product("kn,nqy->kqy", first.imag.astype(np.float32), field)
    real, imag = turn(real, imag, phase(narrow, devices, length, -1)[:, :, None])
    forward = as_blocks(phase(devices, devices, devices, -1))
    spread = product("leq,kqy->leky", forward[..., 0], real) + product(
        "leq,kqy->leky", forward[..., 1], imag
    )
    held = lax.all_to_all(spread, AXES, split_axis=0, concat_axis=0, tiled=True)

    held = product("kesc,scxt->kext", forward, held)
    real, imag = turn(held[:, 0], held[:, 1], phase(devices, narrow, length, -1)[:, None, :])
    hat = product(
        "kxt,tm->kxm",
        jnp.concatenate([real, imag], -1),
        lane_table(phase(narrow, narrow, narrow, -1)),
    )
    hat_real, hat_imag = hat[..., :narrow], hat[..., narrow:]

    ky_index = (
        jnp.arange(devices, dtype=jnp.int32)[:, None, None]
        + devices * jnp.arange(narrow, dtype=jnp.int32)[None, None, :]
    )
    height = centred(ky_index, length)
    across = centred(me * narrow + jnp.arange(narrow, dtype=jnp.int32), length)[None, :, None]
    square_norm = height**2 + across**2
    anchor = square_norm == 0
    safe_norm = jnp.where(anchor, 1.0, square_norm)
    hat_real = jnp.where(anchor, 0.0, hat_real)
    hat_imag = jnp.where(anchor, 0.0, hat_imag)

    kernel_real = (across**2 - height**2) / safe_norm
    kernel_imag = 2.0 * across * height / safe_norm
    shear = jnp.concatenate(
        [
            kernel_real * hat_real - kernel_imag * hat_imag,
            kernel_real * hat_imag + kernel_imag * hat_real,
        ],
        -1,
    )
    back = product(
        "kxm,mt->kxt", shear, lane_table(phase(narrow, narrow, narrow, 1) / length)
    )
    real, imag = turn(
        back[..., :narrow], back[..., narrow:], phase(devices, narrow, length, 1)[:, None, :]
    )
    inverse = as_blocks(phase(devices, devices, devices, 1))
    back = product("sek,kxt->sext", inverse[..., 0], real) + product(
        "sek,kxt->sext", inverse[..., 1], imag
    )
    turned = lax.all_to_all(back, AXES, split_axis=0, concat_axis=0, tiled=True)

    pixel_power = (hat_real**2 + hat_imag**2) * (NBINS / float(length) ** 4)
    bins = spectrum_bin.reshape(narrow, devices, narrow).transpose(1, 2, 0)
    band_ids = jnp.arange(NBINS, dtype=jnp.int32)[:, None, None, None]
    partial_power = jnp.sum(jnp.where(bins == band_ids, pixel_power, 0.0), axis=(1, 2, 3))
    copies = jnp.broadcast_to(partial_power, (devices, 8, NBINS))
    gathered = lax.all_to_all(copies, AXES, split_axis=0, concat_axis=0, tiled=True)
    spectrum = jnp.sum(gathered[:, 0, :], axis=0)

    turned = product("aedc,dcqt->aeqt", inverse, turned)
    real, imag = turn(
        turned[:, 0], turned[:, 1], phase(devices, narrow, length, 1)[:, :, None]
    )
    last = phase(narrow, narrow, narrow, 1) / length
    cos, sin = last.real.astype(np.float32), last.imag.astype(np.float32)
    out_real = product("bq,aqt->bat", cos, real) - product("bq,aqt->bat", sin, imag)
    out_imag = product("bq,aqt->bat", sin, real) + product("bq,aqt->bat", cos, imag)
    shape = (length, narrow)
    return (out_real.reshape(shape).T, out_imag.reshape(shape).T, spectrum)


def folds(mesh, density):
    rows, planes = mesh.shape["rows"], mesh.shape["planes"]
    count, length, width = density.shape
    return (
        count == planes
        and planes == 4
        and length == width == LANES * rows * planes
        and rows * planes == LANES // 4
    )


def solution(mesh):
    specs = (P("planes", "rows", None), P("planes"), P(None, AXES))
    outs = (P(AXES, None), P(AXES, None), P())

    def run(density, lens_weight, spectrum_bin):
        if folds(mesh, density):
            body = folded_device
        else:
            body = on_device
        whole = jax.shard_map(body, mesh=mesh, in_specs=specs, out_specs=outs, check_vma=False)
        return whole(density, lens_weight, spectrum_bin)

    return run
```
